32 devices in a mesh: ens: 2 (over x), part: 4 (over z), feat: 4 (over y, core).
Axes of the slice: x: 2, y: 2, z: 4, core: 2. Of those that a mesh axis runs over, the one named last changes fastest.
Arguments:
- particles: float32 [4096, 12288], P(('ens', 'part'), 'feat'), parts along dimension 0
- prec_diag: float32 [24576], P(('ens', 'feat')), parts along dimension 0
- target_mean: float32 [24576], P(('ens', 'feat')), parts along dimension 0
- low_factor: bfloat16 [24576, 64], P(('ens', 'feat')), parts along dimension 0
Outputs:
- output: float32 [4096, 12288], P(('ens', 'part'), 'feat'), parts along dimension 0
There are 2 independent parts. The reference program is written for one: setup_inputs(seed, part) draws one part's arguments, and reference() takes and returns one part's arrays. A program takes and returns all parts, laid end to end along the dimension named above; each array names one.
All inputs are finite; a program needn't handle non-finite values.
Results may differ from the reference program's by a relative error of at most 0.00351321.
Values are sent between devices in bfloat16 or wider.
A program may use at most 1 GiB of HBM per device.

```python
import math
import jax
import jax.numpy as jnp

NUM_PARTICLES = 2048
FEAT_DIM = 12288
LOW_RANK = 64
NUM_STEPS = 3

KERN_WIDTH = 2.0 * FEAT_DIM / math.log(NUM_PARTICLES)
STEP_SIZE = 0.15 * NUM_PARTICLES * FEAT_DIM / math.log(NUM_PARTICLES)


def setup_inputs(seed: int = 0, part: int = 0) -> dict:
    part_key = jax.random.fold_in(jax.random.key(seed), part)
    sub_keys = jax.random.split(part_key, 6)
    scale_c = math.log(NUM_PARTICLES) / FEAT_DIM
    prec_diag = scale_c * jax.random.uniform(sub_keys[0], (FEAT_DIM,), jnp.float32, 0.5, 1.5)
    low_f32 = (math.sqrt(math.log(NUM_PARTICLES)) / FEAT_DIM) * jax.random.normal(sub_keys[1], (FEAT_DIM, LOW_RANK), jnp.float32)
    low_factor = low_f32.astype(jnp.bfloat16)
    target_mean = 0.5 * jax.random.normal(sub_keys[2], (FEAT_DIM,), jnp.float32)
    offset = 0.5 * jax.random.normal(sub_keys[3], (FEAT_DIM,), jnp.float32)
    spread = math.sqrt(0.5) * jax.random.normal(sub_keys[4], (NUM_PARTICLES, FEAT_DIM), jnp.float32)
    low_coeff = (FEAT_DIM / math.sqrt(2.0 * LOW_RANK * math.log(NUM_PARTICLES))) * jax.random.normal(sub_keys[5], (NUM_PARTICLES, LOW_RANK), jnp.float32)
    low_part = jnp.dot(low_coeff, low_factor.astype(jnp.float32).T)
    particles = target_mean[None, :] + offset[None, :] + spread + low_part
    return {"particles": particles, "prec_diag": prec_diag, "target_mean": target_mean, "low_factor": low_factor}


def svgd_step(cur_theta, prec_diag, target_mean, low_factor):
    x_dev = cur_theta - target_mean[None, :]
    proj_low = jnp.dot(x_dev.astype(jnp.bfloat16), low_factor, preferred_element_type=jnp.float32)
    low_term = jnp.dot(proj_low.astype(jnp.bfloat16), low_factor.T, preferred_element_type=jnp.float32)
    grad_b = (-(x_dev * prec_diag[None, :] + low_term)).astype(jnp.bfloat16)
    theta_b = cur_theta.astype(jnp.bfloat16)
    gram_mat = jnp.dot(theta_b, theta_b.T, preferred_element_type=jnp.float32)
    sq_norm = jnp.sum(jnp.square(theta_b.astype(jnp.float32)), axis=1)
    sq_dist = jnp.maximum(sq_norm[:, None] + sq_norm[None, :] - 2.0 * gram_mat, 0.0)
    kern_b = jnp.exp(-sq_dist / KERN_WIDTH).astype(jnp.bfloat16)
    row_mass = jnp.sum(kern_b.astype(jnp.float32), axis=1)
    drive_term = jnp.dot(kern_b, grad_b, preferred_element_type=jnp.float32)
    pull_term = jnp.dot(kern_b, theta_b, preferred_element_type=jnp.float32)
    update_dir = (drive_term + (2.0 / KERN_WIDTH) * (row_mass[:, None] * theta_b.astype(jnp.float32) - pull_term)) / NUM_PARTICLES
    return cur_theta + STEP_SIZE * update_dir


def reference(particles, prec_diag, target_mean, low_factor):
    cur_theta = particles
    for step_idx in range(NUM_STEPS):
        cur_theta = svgd_step(cur_theta, prec_diag, target_mean, low_factor)
    return cur_theta
```

```python
import math
import jax
import jax.numpy as jnp
from jax import lax
from jax.experimental import pallas as pl
from jax.experimental.pallas import tpu as pltpu
from jax.sharding import PartitionSpec as P

NUM_STEPS = 3
BLK = 128
SPAN = 9
PW = (SPAN + 1) * BLK
GW = SPAN * BLK
NCH = 4
CH = BLK // NCH
TILE = 256
BF = jnp.bfloat16
F32 = jnp.float32
MESH = pl.DeviceIdType.MESH
NT = (((1,), (1,)), ((), ()))


def _dot(a, b):
    return jnp.dot(a, b, preferred_element_type=F32)


def _dot_nt(a, b):
    return lax.dot_general(a, b, NT, preferred_element_type=F32)


def _kernel(n_total, kern_width, step_size,
            theta_in, prec_ref, mean_ref, u0_ref, u1_ref, out_ref,
            th, tb, tsib, ab, gp, fr, cr, zr, kp, k2, zown, zsnd, zrcv, sfull,
            in_s, in_r, tx_s, tx_r, zx_s, zx_r, fy_s, fy_r, ch_s, ch_r, zy_s, zy_r,
            kc_s, kc_r, ky_s, ky_r, kx_s, kx_r, out_s, out_r):
    z = lax.axis_index("part")
    f = lax.axis_index("feat")
    y = f // 2
    c = f % 2
    width = th.shape[1]
    half = n_total // 2
    group = n_total // 4

    def dev(zz, yy, cc):
        return {"part": zz, "feat": 2 * yy + cc}

    me = dev(z, y, c)
    ynb = dev(z, 1 - y, c)
    sib = dev(z, y, 1 - c)
    is_end = jnp.logical_or(z == 0, z == 3)
    is_mid = jnp.logical_not(is_end)
    e1 = jnp.where(z < 2, 1, 0)
    e2 = 1 - e1

    def toward(e):
        return dev(jnp.clip(z + 2 * e - 1, 0, 3), y, c)

    def away(e):
        return dev(jnp.clip(z - 2 * e + 1, 0, 3), y, c)

    def rc(src, dst, ss, rs, d):
        return pltpu.make_async_remote_copy(src_ref=src, dst_ref=dst, send_sem=ss, recv_sem=rs,
                                            device_id=d, device_id_type=MESH)

    bar = pltpu.get_barrier_semaphore()
    for k in range(1, 4):
        pl.semaphore_signal(bar, inc=1, device_id=dev((z + k) % 4, y, c), device_id_type=MESH)
    pl.semaphore_signal(bar, inc=1, device_id=ynb, device_id_type=MESH)
    pl.semaphore_signal(bar, inc=1, device_id=sib, device_id_type=MESH)
    pl.semaphore_wait(bar, 5)

    def grp(zz):
        return pl.multiple_of(((zz + 4 - 2 * c) % 4) * group, group)

    def in_copy(zz):
        return rc(theta_in.at[:, pl.ds(pl.multiple_of(zz * width, BLK), width)], th.at[pl.ds(grp(z), group), :],
                  in_s.at[zz], in_r.at[z], dev(zz, y, c))

    def in_local():
        return pltpu.make_async_copy(theta_in.at[:, pl.ds(pl.multiple_of(z * width, BLK), width)],
                                     th.at[pl.ds(grp(z), group), :], in_r.at[z])

    in_local().start()
    for dist in (3, 2, 1):
        for zz in (z + dist, z - dist):
            @pl.when(jnp.logical_and(zz >= 0, zz < 4))
            def _(zz=zz):
                in_copy(zz).start()

    def t_copy(par, i):
        src = tb.at[par, pl.ds(pl.multiple_of(i * TILE, TILE), TILE), :]
        dst = tsib.at[pl.ds(pl.multiple_of(((i + 4) % 8) * TILE, TILE), TILE), :]
        return rc(src, dst, tx_s.at[i], tx_r.at[(i + 4) % 8], sib)

    def z_copy():
        return rc(zsnd, zrcv, zx_s, zx_r, sib)

    eye = (lax.broadcasted_iota(jnp.int32, (BLK, BLK), 0) == lax.broadcasted_iota(jnp.int32, (BLK, BLK), 1))

    def finish_rows(i, par):
        rows = pl.ds(pl.multiple_of(i * TILE, TILE), TILE)
        tt = th[rows, :].astype(BF)
        tb[par, rows, :] = tt
        t_copy(par, i).start()
        for s in range(TILE // BLK):
            b = i * (TILE // BLK) + s
            t_blk = tt[s * BLK:(s + 1) * BLK].astype(F32)
            s_col = jnp.sum(t_blk * t_blk, axis=1, keepdims=True)
            s_row = jnp.sum(jnp.where(eye, jnp.broadcast_to(s_col, (BLK, BLK)), 0.0), axis=0, keepdims=True)
            zsnd[8, pl.ds(b, 1), :] = s_row
            x_blk = (th[pl.ds(pl.multiple_of(b * BLK, BLK), BLK), :] - mean_ref[...]).astype(BF)
            zq = _dot(x_blk[:BLK // 2], u0_ref[...]) + _dot(x_blk[BLK // 2:], u1_ref[...])

            @pl.when(b < 8)
            def _():
                zown[b] = zq

            @pl.when(b >= 8)
            def _():
                zsnd[b - 8] = zq

    def first_rows(k, carry):
        zz = (z + k) % 4

        @pl.when(k == 0)
        def _():
            in_local().wait()

        @pl.when(k > 0)
        def _():
            rc(th.at[pl.ds(grp(zz), group), :], th.at[pl.ds(grp(zz), group), :], in_s.at[zz], in_r.at[zz], me).wait_recv()
        for s in range(group // TILE):
            finish_rows(((zz + 4 - 2 * c) % 4) * (group // TILE) + s, 0)
        return carry

    lax.fori_loop(0, 4, first_rows, 0)
    z_copy().start()
    for k in range(1, 4):
        in_copy((z + k) % 4).wait_send()

    def qf(yy, e):
        return yy * 2 + e

    def qz(yy, e):
        return 4 + yy * 2 + e

    def crow(i):
        return pl.ds(i * CH, CH)

    def fy_copy(e, i):
        return rc(gp.at[qf(1 - y, e), crow(i), :], fr.at[e, crow(i), :], fy_s.at[e, i], fy_r.at[e, i], ynb)

    def chain_q(n, e):
        return (qz(1 - y, e), qz(y, e), qf(y, e))[n // NCH]

    def chain_copy(n, e):
        return rc(gp.at[chain_q(n, e), crow(n % NCH), :], cr.at[e, n], ch_s.at[e, n], ch_r.at[e, n], toward(e))

    def zy_copy(i):
        return rc(gp.at[qz(1 - y, e2), crow(i), :], zr.at[crow(i), :], zy_s.at[i], zy_r.at[i], ynb)

    HR = BLK // 2

    def krow(ch):
        return pl.ds(ch * HR, HR)

    def kc_copy(e, j, ch, q):
        return rc(kp.at[0, q, krow(ch), :], kp.at[0, q, krow(ch), :], kc_s.at[e, j * 2 + ch], kc_r.at[e, j * 2 + ch], away(e))

    def ky_copy(e, kind, ch, q):
        return rc(kp.at[0, q, krow(ch), :], kp.at[0, q, krow(ch), :], ky_s.at[e, kind, ch], ky_r.at[e, kind, ch], ynb)

    def kx_copy(ch, q):
        return rc(kp.at[0, q, krow(ch), :], kp.at[1, q, krow(ch), :], kx_s.at[q, ch], kx_r.at[q, ch], sib)

    def step(t, carry):
        par = t % 2

        def t_wait(i, cc):
            t_copy(par, i).wait()
            return cc

        lax.fori_loop(0, 8, t_wait, 0)
        z_copy().wait()
        sfull[0:8, :] = zsnd[8, 0:8, :] + zrcv[8, 8:16, :]
        sfull[8:16, :] = zsnd[8, 8:16, :] + zrcv[8, 0:8, :]

        def panel(q):
            rows = pl.ds(pl.multiple_of(q * BLK, BLK), BLK)
            win = pl.ds(pl.multiple_of(q * BLK, BLK), GW)
            gp[q, :, 0:GW] = _dot_nt(tb[par, rows, :], tb[par, win, :]) + _dot_nt(tsib[rows, :], tsib[win, :])
            gp[q, 0:16, GW:PW] = sfull[...]
            gp[q, 16:80, GW:PW] = zown[q] + zrcv[q]
            gp[q, 80:BLK, GW:PW] = jnp.zeros((BLK - 80, BLK), F32)

        def mk_panels(m, cc):
            e = jnp.where(m % 2 == 0, e1, e2)
            g = m // 2
            q = jnp.where(g == 0, qf(1 - y, e), jnp.where(g == 1, qz(1 - y, e), jnp.where(g == 2, qz(y, e), qf(y, e))))
            panel(q)

            @pl.when(g == 0)
            def _():
                for i in range(NCH):
                    fy_copy(e, i).start()

            for gg in (1, 2):
                @pl.when(jnp.logical_and(is_end, m == 2 * gg))
                def _(gg=gg):
                    for i in range(NCH):
                        chain_copy((gg - 1) * NCH + i, e1).start()
            return cc

        lax.fori_loop(0, 8, mk_panels, 0)

        def kern_panel(q):
            s_col = jnp.sum(jnp.where(eye, jnp.broadcast_to(sfull[pl.ds(q, 1), :], (BLK, BLK)), 0.0), axis=1, keepdims=True)
            for k in range(SPAN):
                cols = slice(k * BLK, (k + 1) * BLK)
                dist = jnp.maximum(s_col + sfull[pl.ds(q + k, 1), :] - 2.0 * gp[q, :, cols], 0.0)
                kp[0, q, :, cols] = jnp.exp(dist * (-1.0 / kern_width)).astype(BF)
            kp[0, q, 0:HR, GW:PW] = jnp.zeros((HR, BLK), BF)
            kp[0, q, HR:BLK, GW:PW] = gp[q, 16:80, GW:PW].astype(BF)

        def send_own(j, q):
            for ch in range(2):
                kc_copy(e2, j, ch, q).start()
                ky_copy(e2, 1 - j, ch, q).start()
                kx_copy(ch, q).start()

        for n in range(3 * NCH):
            i = n % NCH
            rows = crow(i)

            def take(e, with_chain, with_y):
                q = chain_q(n, e)
                val = gp[q, rows, :]
                if with_y:
                    fy_copy_in = rc(fr.at[e, rows, :], fr.at[e, rows, :], fy_s.at[e, i], fy_r.at[e, i], ynb)
                    fy_copy_in.wait_recv()
                    val = val + fr[e, rows, :]
                if with_chain:
                    rc(cr.at[e, n], cr.at[e, n], ch_s.at[e, n], ch_r.at[e, n], me).wait_recv()
                    val = val + cr[e, n]
                gp[q, rows, :] = val

            @pl.when(is_mid)
            def _(n=n, take=take):
                for e in (e1, e2):
                    take(e, True, n >= 2 * NCH)
                    chain_copy(n, e).start()

            @pl.when(is_end)
            def _(n=n, i=i, take=take, rows=rows):
                if n >= 2 * NCH:
                    take(e1, False, True)
                    chain_copy(n, e1).start()
                take(e2, True, n >= 2 * NCH)
                if n < NCH:
                    zy_copy(i).start()
                elif n < 2 * NCH:
                    rc(zr.at[rows, :], zr.at[rows, :], zy_s.at[i], zy_r.at[i], me).wait_recv()
                    q = qz(y, e2)
                    gp[q, rows, :] = gp[q, rows, :] + zr[rows, :]
                if n == 2 * NCH - 1:
                    q = qz(y, e2)
                    sfull[...] = gp[q, 0:16, GW:PW]
                    kern_panel(q)
                    send_own(0, q)
                if n == 3 * NCH - 1:
                    q = qf(y, e2)
                    kern_panel(q)
                    send_own(1, q)

        def assemble(h, q):
            lo = pl.ds(pl.multiple_of(q * BLK, BLK), BLK)
            for k in range(SPAN):
                blk = kp[h, q, :, k * BLK:(k + 1) * BLK]
                k2[h, lo, pl.ds(pl.multiple_of((q + k) * BLK, BLK), BLK)] = blk
                if 1 <= k <= 7:
                    flip = (q + k) // 8
                    k2[(h + flip) % 2, pl.ds(pl.multiple_of((q + k - 8 * flip) * BLK, BLK), BLK),
                       pl.ds(pl.multiple_of((q + 8 * flip) * BLK, BLK), BLK)] = blk.T
            zb = kp[h, q, HR:BLK, GW:PW]
            for s, u_ref in ((0, u0_ref), (1, u1_ref)):
                rows = pl.ds(pl.multiple_of((h * 8 + q) * BLK + s * HR, HR), HR)
                low = _dot_nt(zb, u_ref[...])
                x_dev = th[rows, :] - mean_ref[...]
                ab[rows, :] = (-(x_dev * prec_ref[...] + low)).astype(BF)

        def slot_q(slot):
            j = slot // 2
            e = jnp.where(slot % 2 == 0, e2, e1)
            q = jnp.where(j == 0, qz(y, e), jnp.where(j == 1, qf(y, e), jnp.where(j == 2, qz(1 - y, e), qf(1 - y, e))))
            return j, e, q

        def slot_body(slot, cc):
            @pl.when(slot < 8)
            def _():
                j, e, q = slot_q(slot)
                at_origin = jnp.logical_and(is_end, e == e2)
                own = jnp.logical_and(at_origin, j < 2)
                from_y = jnp.logical_or(j == 3, jnp.logical_and(at_origin, j == 2))
                from_chain = jnp.logical_not(jnp.logical_or(own, from_y))
                last = jnp.logical_and(is_end, e == e1)
                fwd = jnp.logical_and(jnp.logical_and(j < 3, jnp.logical_not(last)), jnp.logical_not(own))
                kind = jnp.where(j == 3, 0, 1)
                for ch in range(2):
                    buf = kp.at[0, q, krow(ch), :]

                    @pl.when(from_chain)
                    def _():
                        jj = jnp.minimum(j, 2)
                        rc(buf, buf, kc_s.at[e, jj * 2 + ch], kc_r.at[e, jj * 2 + ch], me).wait_recv()

                    @pl.when(from_y)
                    def _():
                        rc(buf, buf, ky_s.at[e, kind, ch], ky_r.at[e, kind, ch], me).wait_recv()

                    @pl.when(fwd)
                    def _():
                        kc_copy(e, j, ch, q).start()

                    @pl.when(jnp.logical_and(j == 1, jnp.logical_not(own)))
                    def _():
                        ky_copy(e, 0, ch, q).start()

                    @pl.when(jnp.logical_not(own))
                    def _():
                        kx_copy(ch, q).start()
                assemble(0, q)

            @pl.when(slot > 0)
            def _():
                _, _, q = slot_q(slot - 1)
                for ch in range(2):
                    buf = kp.at[1, q, krow(ch), :]
                    rc(buf, buf, kx_s.at[q, ch], kx_r.at[q, ch], me).wait_recv()
                assemble(1, q)
            return cc

        lax.fori_loop(0, 9, slot_body, 0)

        for e in range(2):
            for i in range(NCH):
                fy_copy(e, i).wait_send()
        for n in range(3 * NCH):
            chain_copy(n, e1).wait_send()

            @pl.when(is_mid)
            def _(n=n):
                chain_copy(n, e2).wait_send()

        @pl.when(is_end)
        def _():
            for i in range(NCH):
                zy_copy(i).wait_send()

        def phi_tile(i, cc):
            h = i // 4
            rows = pl.ds(pl.multiple_of(i * TILE, TILE), TILE)
            krows = pl.ds(pl.multiple_of((i % 4) * TILE, TILE), TILE)
            first = pl.ds(pl.multiple_of(h * half, half), half)
            second = pl.ds(pl.multiple_of((1 - h) * half, half), half)
            ka = k2[h, krows, 0:half]
            kb = k2[h, krows, half:n_total]
            drive = _dot(ka, ab[first, :]) + _dot(kb, ab[second, :])
            pull = _dot(ka, tb[par, first, :]) + _dot(kb, tb[par, second, :])
            mass = jnp.sum(ka.astype(F32), axis=1, keepdims=True) + jnp.sum(kb.astype(F32), axis=1, keepdims=True)
            t_own = tb[par, rows, :].astype(F32)
            upd = (drive + (2.0 / kern_width) * (mass * t_own - pull)) * (1.0 / n_total)
            th[rows, :] = th[rows, :] + step_size * upd

            @pl.when(t < NUM_STEPS - 1)
            def _():
                finish_rows(i, 1 - par)

            @pl.when(t == NUM_STEPS - 1)
            def _():
                zz = (i // 2 + 2 * c) % 4
                dst = out_ref.at[pl.ds(pl.multiple_of((i % 2) * TILE, TILE), TILE), pl.ds(pl.multiple_of(z * width, BLK), width)]

                @pl.when(zz == z)
                def _():
                    pltpu.make_async_copy(th.at[rows, :], dst, out_s.at[i]).start()

                @pl.when(zz != z)
                def _():
                    rc(th.at[rows, :], dst, out_s.at[i], out_r.at[z, i % 2], dev(zz, y, c)).start()
            return cc

        lax.fori_loop(0, 8, phi_tile, 0)

        @pl.when(t < NUM_STEPS - 1)
        def _():
            z_copy().start()

        for ch in range(2):
            for e in range(2):
                ky_copy(e, 0, ch, qf(y, e)).wait_send()

            @pl.when(is_end)
            def _(ch=ch):
                ky_copy(e2, 1, ch, qz(y, e2)).wait_send()
            for j in range(3):
                q2 = (qz(y, e2), qf(y, e2), qz(1 - y, e2))[j]
                q1 = (qz(y, e1), qf(y, e1), qz(1 - y, e1))[j]
                kc_copy(e2, j, ch, q2).wait_send()

                @pl.when(is_mid)
                def _(ch=ch, j=j, q1=q1):
                    kc_copy(e1, j, ch, q1).wait_send()
            for q in range(8):
                kx_copy(ch, q).wait_send()
        return carry

    lax.fori_loop(0, NUM_STEPS, step, 0)

    def out_wait(i, cc):
        zz = (i // 2 + 2 * c) % 4
        rows = pl.ds(pl.multiple_of(i * TILE, TILE), TILE)
        dst = out_ref.at[pl.ds(pl.multiple_of((i % 2) * TILE, TILE), TILE), pl.ds(pl.multiple_of(z * width, BLK), width)]

        @pl.when(zz == z)
        def _():
            pltpu.make_async_copy(th.at[rows, :], dst, out_s.at[i]).wait()

        @pl.when(zz != z)
        def _():
            rc(th.at[rows, :], dst, out_s.at[i], out_r.at[z, i % 2], dev(zz, y, c)).wait_send()
        return cc

    lax.fori_loop(0, 8, out_wait, 0)
    for k in range(1, 4):
        zz = (z + k) % 4
        for s in range(2):
            dst = out_ref.at[pl.ds(s * TILE, TILE), pl.ds(pl.multiple_of(zz * width, BLK), width)]
            rc(dst, dst, out_s.at[0], out_r.at[zz, s], me).wait_recv()


def solution(mesh):
    part_size = mesh.shape["part"]
    feat_size = mesh.shape["feat"]

    def local_steps(local_theta, prec_loc, mean_loc, factor_loc):
        rows_loc, feat_loc = local_theta.shape
        n_total = rows_loc * part_size
        feat_total = feat_loc * feat_size
        width = feat_loc // part_size
        kern_width = 2.0 * feat_total / math.log(n_total)
        step_size = 0.15 * n_total * feat_total / math.log(n_total)
        start = lax.axis_index("part") * width
        prec = lax.dynamic_slice_in_dim(prec_loc, start, width)[None, :]
        mean = lax.dynamic_slice_in_dim(mean_loc, start, width)[None, :]
        factor = lax.dynamic_slice_in_dim(factor_loc, start, width)
        rank = factor.shape[1]
        u0 = jnp.pad(factor, ((0, 0), (0, BLK - rank)))
        u1 = jnp.pad(factor, ((0, 0), (BLK - rank, 0)))
        vmem = pl.BlockSpec(memory_space=pltpu.VMEM)
        anym = pl.BlockSpec(memory_space=pl.ANY)
        dma = pltpu.SemaphoreType.DMA
        body = lambda *refs: _kernel(n_total, kern_width, step_size, *refs)
        return pl.pallas_call(
            body,
            out_shape=jax.ShapeDtypeStruct((rows_loc, feat_loc), F32),
            in_specs=[anym, vmem, vmem, vmem, vmem],
            out_specs=anym,
            scratch_shapes=[
                pltpu.VMEM((n_total, width), F32),
                pltpu.VMEM((2, n_total, width), BF),
                pltpu.VMEM((n_total, width), BF),
                pltpu.VMEM((n_total, width), BF),
                pltpu.VMEM((8, BLK, PW), F32),
                pltpu.VMEM((2, BLK, PW), F32),
                pltpu.VMEM((2, 3 * NCH, CH, PW), F32),
                pltpu.VMEM((BLK, PW), F32),
                pltpu.VMEM((2, 8, BLK, PW), BF),
                pltpu.VMEM((2, n_total // 2, n_total), BF),
                pltpu.VMEM((8, BLK // 2, BLK), F32),
                pltpu.VMEM((9, BLK // 2, BLK), F32),
                pltpu.VMEM((9, BLK // 2, BLK), F32),
                pltpu.VMEM((16, BLK), F32),
                dma((4,)), dma((4,)), dma((8,)), dma((8,)), dma, dma,
                dma((2, NCH)), dma((2, NCH)), dma((2, 3 * NCH)), dma((2, 3 * NCH)), dma((NCH,)), dma((NCH,)),
                dma((2, 6)), dma((2, 6)), dma((2, 2, 2)), dma((2, 2, 2)), dma((8, 2)), dma((8, 2)),
                dma((8,)), dma((4, 2)),
            ],
            compiler_params=pltpu.CompilerParams(collective_id=0, has_side_effects=True, vmem_limit_bytes=63 * 1024 * 1024),
            name="svgd",
        )(local_theta, prec, mean, u0, u1)

    row_spec = P(("ens", "part"), "feat")
    vec_spec = P(("ens", "feat"))
    fac_spec = P(("ens", "feat"), None)
    return jax.shard_map(local_steps, mesh=mesh, in_specs=(row_spec, vec_spec, vec_spec, fac_spec), out_specs=row_spec, check_vma=False)
```

```python
import math
import jax
import jax.numpy as jnp
from jax import lax
from jax.experimental import pallas as pl
from jax.experimental.pallas import tpu as pltpu
from jax.sharding import PartitionSpec as P

NUM_STEPS = 3
BLK = 128
SPAN = 9
PW = (SPAN + 1) * BLK
GW = SPAN * BLK
NCH = 8
CH = BLK // NCH
KCH = 4
HR = BLK // 2
KSKEW = 2
SKEW = 3
TILE = 256
BF = jnp.bfloat16
F32 = jnp.float32
MESH = pl.DeviceIdType.MESH
NT = (((1,), (1,)), ((), ()))


def _dot(a, b):
    return jnp.dot(a, b, preferred_element_type=F32)


def _dot_nt(a, b):
    return lax.dot_general(a, b, NT, preferred_element_type=F32)


def _kernel(n_total, kern_width, step_size,
            theta_in, prec_ref, mean_ref, u0_ref, u1_ref, out_ref,
            th, tb, tsib, ab, gp, fr, cr, zr, kp, k2, zown, zsnd, zrcv, sfull,
            in_s, in_r, tx_s, tx_r, zx_s, zx_r, fy_s, fy_r, ch_s, ch_r, zy_s, zy_r,
            kc_s, kc_r, ky_s, ky_r, kx_s, kx_r, out_s, out_r):
    z = lax.axis_index("part")
    f = lax.axis_index("feat")
    y = f // 2
    c = f % 2
    width = th.shape[1]
    half = n_total // 2
    group = n_total // 4

    def dev(zz, yy, cc):
        return {"part": zz, "feat": 2 * yy + cc}

    me = dev(z, y, c)
    ynb = dev(z, 1 - y, c)
    sib = dev(z, y, 1 - c)
    is_end = jnp.logical_or(z == 0, z == 3)
    is_mid = jnp.logical_not(is_end)
    e1 = jnp.where(z < 2, 1, 0)
    e2 = 1 - e1

    def toward(e):
        return dev(jnp.clip(z + 2 * e - 1, 0, 3), y, c)

    def away(e):
        return dev(jnp.clip(z - 2 * e + 1, 0, 3), y, c)

    def rc(src, dst, ss, rs, d):
        return pltpu.make_async_remote_copy(src_ref=src, dst_ref=dst, send_sem=ss, recv_sem=rs,
                                            device_id=d, device_id_type=MESH)

    bar = pltpu.get_barrier_semaphore()
    for k in range(1, 4):
        pl.semaphore_signal(bar, inc=1, device_id=dev((z + k) % 4, y, c), device_id_type=MESH)
    pl.semaphore_signal(bar, inc=1, device_id=ynb, device_id_type=MESH)
    pl.semaphore_signal(bar, inc=1, device_id=sib, device_id_type=MESH)
    pl.semaphore_wait(bar, 5)

    def grp(zz):
        return pl.multiple_of(((zz + 4 - 2 * c) % 4) * group, group)

    def in_copy(zz):
        return rc(theta_in.at[:, pl.ds(pl.multiple_of(zz * width, BLK), width)], th.at[pl.ds(grp(z), group), :],
                  in_s.at[zz], in_r.at[z], dev(zz, y, c))

    def in_local():
        return pltpu.make_async_copy(theta_in.at[:, pl.ds(pl.multiple_of(z * width, BLK), width)],
                                     th.at[pl.ds(grp(z), group), :], in_r.at[z])

    in_local().start()
    for dist in (3, 2, 1):
        for zz in (z + dist, z - dist):
            @pl.when(jnp.logical_and(zz >= 0, zz < 4))
            def _(zz=zz):
                in_copy(zz).start()

    def t_copy(par, i):
        src = tb.at[par, pl.ds(pl.multiple_of(i * TILE, TILE), TILE), :]
        dst = tsib.at[pl.ds(pl.multiple_of(((i + 4) % 8) * TILE, TILE), TILE), :]
        return rc(src, dst, tx_s.at[i], tx_r.at[(i + 4) % 8], sib)

    def z_copy():
        return rc(zsnd, zrcv, zx_s, zx_r, sib)

    eye = (lax.broadcasted_iota(jnp.int32, (BLK, BLK), 0) == lax.broadcasted_iota(jnp.int32, (BLK, BLK), 1))

    def finish_rows(i, par):
        rows = pl.ds(pl.multiple_of(i * TILE, TILE), TILE)
        tt = th[rows, :].astype(BF)
        tb[par, rows, :] = tt
        t_copy(par, i).start()
        for s in range(TILE // BLK):
            b = i * (TILE // BLK) + s
            t_blk = tt[s * BLK:(s + 1) * BLK].astype(F32)
            s_col = jnp.sum(t_blk * t_blk, axis=1, keepdims=True)
            s_row = jnp.sum(jnp.where(eye, jnp.broadcast_to(s_col, (BLK, BLK)), 0.0), axis=0, keepdims=True)
            zsnd[8, pl.ds(b, 1), :] = s_row
            x_blk = (th[pl.ds(pl.multiple_of(b * BLK, BLK), BLK), :] - mean_ref[...]).astype(BF)
            zq = _dot(x_blk[:BLK // 2], u0_ref[...]) + _dot(x_blk[BLK // 2:], u1_ref[...])

            @pl.when(b < 8)
            def _():
                zown[b] = zq

            @pl.when(b >= 8)
            def _():
                zsnd[b - 8] = zq

    def first_rows(k, carry):
        zz = (z + k) % 4

        @pl.when(k == 0)
        def _():
            in_local().wait()

        @pl.when(k > 0)
        def _():
            rc(th.at[pl.ds(grp(zz), group), :], th.at[pl.ds(grp(zz), group), :], in_s.at[zz], in_r.at[zz], me).wait_recv()
        for s in range(group // TILE):
            finish_rows(((zz + 4 - 2 * c) % 4) * (group // TILE) + s, 0)
        return carry

    lax.fori_loop(0, 4, first_rows, 0)
    z_copy().start()
    for k in range(1, 4):
        in_copy((z + k) % 4).wait_send()

    def qf(yy, e):
        return yy * 2 + e

    def qz(yy, e):
        return 4 + yy * 2 + e

    def crow(i):
        return pl.ds(i * CH, CH)

    def fy_copy(e, i):
        return rc(gp.at[qf(1 - y, e), crow(i), :], fr.at[e, crow(i), :], fy_s.at[e, i], fy_r.at[e, i], ynb)

    def chain_q(n, e):
        return (qz(1 - y, e), qz(y, e), qf(y, e))[n // NCH]

    def chain_copy(n, e):
        return rc(gp.at[chain_q(n, e), crow(n % NCH), :], cr.at[e, n], ch_s.at[e, n], ch_r.at[e, n], toward(e))

    def zy_copy(i):
        return rc(gp.at[qz(1 - y, e2), crow(i), :], zr.at[crow(i), :], zy_s.at[i], zy_r.at[i], ynb)

    def krow(ch):
        return pl.ds(ch * (BLK // KCH), BLK // KCH)

    def kc_copy(e, j, ch, q):
        return rc(kp.at[0, q, krow(ch), :], kp.at[0, q, krow(ch), :], kc_s.at[e, j * KCH + ch], kc_r.at[e, j * KCH + ch], away(e))

    def ky_copy(e, kind, ch, q):
        return rc(kp.at[0, q, krow(ch), :], kp.at[0, q, krow(ch), :], ky_s.at[e, kind, ch], ky_r.at[e, kind, ch], ynb)

    def kx_copy(ch, q):
        return rc(kp.at[0, q, krow(ch), :], kp.at[1, q, krow(ch), :], kx_s.at[q, ch], kx_r.at[q, ch], sib)

    def step(t, carry):
        par = t % 2

        def t_wait(i, cc):
            t_copy(par, i).wait()
            return cc

        lax.fori_loop(0, 8, t_wait, 0)
        z_copy().wait()
        sfull[0:8, :] = zsnd[8, 0:8, :] + zrcv[8, 8:16, :]
        sfull[8:16, :] = zsnd[8, 8:16, :] + zrcv[8, 0:8, :]

        def panel(q):
            rows = pl.ds(pl.multiple_of(q * BLK, BLK), BLK)
            win = pl.ds(pl.multiple_of(q * BLK, BLK), GW)
            gp[q, :, 0:GW] = _dot_nt(tb[par, rows, :], tb[par, win, :]) + _dot_nt(tsib[rows, :], tsib[win, :])
            gp[q, 0:16, GW:PW] = sfull[...]
            gp[q, 16:80, GW:PW] = zown[q] + zrcv[q]
            gp[q, 80:BLK, GW:PW] = jnp.zeros((BLK - 80, BLK), F32)

        def mk_panels(m, cc):
            k = jnp.where(is_end, jnp.where(m == 0, 2, jnp.where(m < 3, m - 1, 3)), m)
            e = jnp.where(k % 2 == 0, e1, e2)
            panel(jnp.where(k < 2, qf(1 - y, e), qz(1 - y, e)))

            @pl.when(k < 2)
            def _():
                for i in range(NCH):
                    fy_copy(e, i).start()

            @pl.when(jnp.logical_and(is_end, m == 0))
            def _():
                for i in range(NCH):
                    chain_copy(i, e1).start()
            return cc

        lax.fori_loop(0, 4, mk_panels, 0)

        def late_panels(m, cc):
            e = jnp.where(m % 2 == 0, e1, e2)
            panel(jnp.where(m < 2, qz(y, e), qf(y, e)))

            @pl.when(jnp.logical_and(is_end, m == 0))
            def _():
                for i in range(NCH):
                    chain_copy(NCH + i, e1).start()
            return cc

        def kern_panel(q):
            s_col = jnp.sum(jnp.where(eye, jnp.broadcast_to(sfull[pl.ds(q, 1), :], (BLK, BLK)), 0.0), axis=1, keepdims=True)
            for k in range(SPAN):
                cols = slice(k * BLK, (k + 1) * BLK)
                dist = jnp.maximum(s_col + sfull[pl.ds(q + k, 1), :] - 2.0 * gp[q, :, cols], 0.0)
                kp[0, q, :, cols] = jnp.exp(dist * (-1.0 / kern_width)).astype(BF)
            kp[0, q, 0:HR, GW:PW] = jnp.zeros((HR, BLK), BF)
            kp[0, q, HR:BLK, GW:PW] = gp[q, 16:80, GW:PW].astype(BF)

        def send_own(j, q):
            for ch in range(KCH):
                kc_copy(e2, j, ch, q).start()
                ky_copy(e2, 1 - j, ch, q).start()
                kx_copy(ch, q).start()

        def take(n, e, with_chain, with_y):
            i = n % NCH
            rows = crow(i)
            q = chain_q(n, e)
            val = gp[q, rows, :]
            if with_y:
                rc(fr.at[e, rows, :], fr.at[e, rows, :], fy_s.at[e, i], fy_r.at[e, i], me).wait_recv()
                val = val + fr[e, rows, :]
            if with_chain:
                rc(cr.at[e, n], cr.at[e, n], ch_s.at[e, n], ch_r.at[e, n], me).wait_recv()
                val = val + cr[e, n]
            gp[q, rows, :] = val

        def mid_round(m):
            for n, e in ((m, e1), (m - SKEW, e2)):
                if 0 <= n < 3 * NCH:
                    take(n, e, True, n >= 2 * NCH)
                    chain_copy(n, e).start()

        def end_round(n):
            i = n % NCH
            rows = crow(i)
            if NCH <= n < 2 * NCH:
                take(n + NCH, e1, False, True)
                chain_copy(n + NCH, e1).start()
            take(n, e2, True, n >= 2 * NCH)
            if n < NCH:
                zy_copy(i).start()
            elif n < 2 * NCH:
                rc(zr.at[rows, :], zr.at[rows, :], zy_s.at[i], zy_r.at[i], me).wait_recv()
                q = qz(y, e2)
                gp[q, rows, :] = gp[q, rows, :] + zr[rows, :]
            if n == 2 * NCH - 1:
                q = qz(y, e2)
                sfull[...] = gp[q, 0:16, GW:PW]
                kern_panel(q)
                send_own(0, q)
            if n == 3 * NCH - 1:
                q = qf(y, e2)
                kern_panel(q)
                send_own(1, q)

        @pl.when(is_mid)
        def _():
            for m in range(3 * NCH + SKEW):
                if m < 4:
                    lax.fori_loop(m, m + 1, late_panels, 0)
                mid_round(m)

        @pl.when(is_end)
        def _():
            lax.fori_loop(0, 4, late_panels, 0)
            for n in range(3 * NCH):
                end_round(n)

        def assemble(h, q):
            lo = pl.ds(pl.multiple_of(q * BLK, BLK), BLK)
            for k in range(SPAN):
                blk = kp[h, q, :, k * BLK:(k + 1) * BLK]
                k2[h, lo, pl.ds(pl.multiple_of((q + k) * BLK, BLK), BLK)] = blk
                if 1 <= k <= 7:
                    flip = (q + k) // 8
                    k2[(h + flip) % 2, pl.ds(pl.multiple_of((q + k - 8 * flip) * BLK, BLK), BLK),
                       pl.ds(pl.multiple_of((q + 8 * flip) * BLK, BLK), BLK)] = blk.T
            zb = kp[h, q, HR:BLK, GW:PW]
            for s, u_ref in ((0, u0_ref), (1, u1_ref)):
                rows = pl.ds(pl.multiple_of((h * 8 + q) * BLK + s * HR, HR), HR)
                low = _dot_nt(zb, u_ref[...])
                x_dev = th[rows, :] - mean_ref[...]
                ab[rows, :] = (-(x_dev * prec_ref[...] + low)).astype(BF)

        def panel_q(j, e):
            return jnp.where(j == 0, qz(y, e), jnp.where(j == 1, qf(y, e), qz(1 - y, e)))

        def k_take(m, e, fwd):
            j, ch = m // KCH, m % KCH
            q = panel_q(j, e)
            rows = pl.ds(pl.multiple_of(ch * (BLK // KCH), BLK // KCH), BLK // KCH)
            buf = kp.at[0, q, rows, :]
            rc(buf, buf, kc_s.at[e, m], kc_r.at[e, m], me).wait_recv()
            if fwd:
                rc(buf, buf, kc_s.at[e, m], kc_r.at[e, m], away(e)).start()

            @pl.when(j == 1)
            def _():
                rc(buf, buf, ky_s.at[e, 0, ch], ky_r.at[e, 0, ch], ynb).start()
            rc(buf, kp.at[1, q, rows, :], kx_s.at[q, ch], kx_r.at[q, ch], sib).start()

        def from_sib(q):
            for ch in range(KCH):
                buf = kp.at[1, q, krow(ch), :]
                rc(buf, buf, kx_s.at[q, ch], kx_r.at[q, ch], me).wait_recv()
            assemble(1, q)

        def from_y(e):
            q = qf(1 - y, e)
            for ch in range(KCH):
                buf = kp.at[0, q, krow(ch), :]
                rc(buf, buf, ky_s.at[e, 0, ch], ky_r.at[e, 0, ch], me).wait_recv()
                kx_copy(ch, q).start()
            assemble(0, q)

        @pl.when(is_end)
        def _():
            q = qz(1 - y, e2)
            for ch in range(KCH):
                buf = kp.at[0, q, krow(ch), :]
                rc(buf, buf, ky_s.at[e2, 1, ch], ky_r.at[e2, 1, ch], me).wait_recv()
                kc_copy(e2, 2, ch, q).start()
                kx_copy(ch, q).start()

        def k_round(m, cc):
            near = m < 3 * KCH
            far = m >= KSKEW
            nf = jnp.maximum(m - KSKEW, 0)
            nn = jnp.minimum(m, 3 * KCH - 1)

            @pl.when(jnp.logical_and(near, is_mid))
            def _():
                k_take(nn, e2, True)

            @pl.when(jnp.logical_and(far, is_mid))
            def _():
                k_take(nf, e1, True)

            @pl.when(jnp.logical_and(far, is_end))
            def _():
                k_take(nf, e1, False)

            @pl.when(jnp.logical_and(near, m % KCH == KCH - 1))
            def _():
                assemble(0, panel_q(nn // KCH, e2))

            @pl.when(jnp.logical_and(near, jnp.logical_and(m % KCH == KCH - 1, m >= KCH)))
            def _():
                from_sib(panel_q(nn // KCH - 1, e2))

            @pl.when(jnp.logical_and(far, nf % KCH == KCH - 1))
            def _():
                assemble(0, panel_q(nf // KCH, e1))

            @pl.when(jnp.logical_and(far, jnp.logical_and(nf % KCH == KCH - 1, nf >= KCH)))
            def _():
                from_sib(panel_q(nf // KCH - 1, e1))

            @pl.when(m == 2 * KCH + KSKEW)
            def _():
                from_y(e2)
            return cc

        lax.fori_loop(0, 3 * KCH + KSKEW, k_round, 0)
        from_y(e1)

        def last_sib(k, cc):
            from_sib(jnp.where(k == 0, panel_q(2, e2), jnp.where(k == 1, qf(1 - y, e2), jnp.where(k == 2, qf(1 - y, e1), panel_q(2, e1)))))
            return cc

        lax.fori_loop(0, 4, last_sib, 0)

        for e in range(2):
            for i in range(NCH):
                fy_copy(e, i).wait_send()
        for n in range(3 * NCH):
            chain_copy(n, e1).wait_send()

            @pl.when(is_mid)
            def _(n=n):
                chain_copy(n, e2).wait_send()

        @pl.when(is_end)
        def _():
            for i in range(NCH):
                zy_copy(i).wait_send()

        def phi_tile(k, cc):
            low = z < 2
            zm = jnp.where(low, z, 3 - z)
            zo = jnp.where(k < 2, 2, jnp.where(k < 4, 3, jnp.where(k < 6, 1 - zm, zm)))
            zz = jnp.where(low, zo, 3 - zo)
            i = ((zz + 4 - 2 * c) % 4) * 2 + k % 2
            h = i // 4
            rows = pl.ds(pl.multiple_of(i * TILE, TILE), TILE)
            krows = pl.ds(pl.multiple_of((i % 4) * TILE, TILE), TILE)
            first = pl.ds(pl.multiple_of(h * half, half), half)
            second = pl.ds(pl.multiple_of((1 - h) * half, half), half)
            ka = k2[h, krows, 0:half]
            kb = k2[h, krows, half:n_total]
            drive = _dot(ka, ab[first, :]) + _dot(kb, ab[second, :])
            pull = _dot(ka, tb[par, first, :]) + _dot(kb, tb[par, second, :])
            mass = jnp.sum(ka.astype(F32), axis=1, keepdims=True) + jnp.sum(kb.astype(F32), axis=1, keepdims=True)
            t_own = tb[par, rows, :].astype(F32)
            upd = (drive + (2.0 / kern_width) * (mass * t_own - pull)) * (1.0 / n_total)
            th[rows, :] = th[rows, :] + step_size * upd

            @pl.when(t < NUM_STEPS - 1)
            def _():
                finish_rows(i, 1 - par)

            @pl.when(t == NUM_STEPS - 1)
            def _():
                dst = out_ref.at[pl.ds(pl.multiple_of((i % 2) * TILE, TILE), TILE), pl.ds(pl.multiple_of(z * width, BLK), width)]

                @pl.when(zz == z)
                def _():
                    pltpu.make_async_copy(th.at[rows, :], dst, out_s.at[i]).start()

                @pl.when(zz != z)
                def _():
                    rc(th.at[rows, :], dst, out_s.at[i], out_r.at[z, i % 2], dev(zz, y, c)).start()
            return cc

        lax.fori_loop(0, 8, phi_tile, 0)

        @pl.when(t < NUM_STEPS - 1)
        def _():
            z_copy().start()

        for ch in range(KCH):
            for e in range(2):
                ky_copy(e, 0, ch, qf(y, e)).wait_send()

            @pl.when(is_end)
            def _(ch=ch):
                ky_copy(e2, 1, ch, qz(y, e2)).wait_send()
            for j in range(3):
                q2 = (qz(y, e2), qf(y, e2), qz(1 - y, e2))[j]
                q1 = (qz(y, e1), qf(y, e1), qz(1 - y, e1))[j]
                kc_copy(e2, j, ch, q2).wait_send()

                @pl.when(is_mid)
                def _(ch=ch, j=j, q1=q1):
                    kc_copy(e1, j, ch, q1).wait_send()
            for q in range(8):
                kx_copy(ch, q).wait_send()
        return carry

    lax.fori_loop(0, NUM_STEPS, step, 0)

    def out_wait(i, cc):
        zz = (i // 2 + 2 * c) % 4
        rows = pl.ds(pl.multiple_of(i * TILE, TILE), TILE)
        dst = out_ref.at[pl.ds(pl.multiple_of((i % 2) * TILE, TILE), TILE), pl.ds(pl.multiple_of(z * width, BLK), width)]

        @pl.when(zz == z)
        def _():
            pltpu.make_async_copy(th.at[rows, :], dst, out_s.at[i]).wait()

        @pl.when(zz != z)
        def _():
            rc(th.at[rows, :], dst, out_s.at[i], out_r.at[z, i % 2], dev(zz, y, c)).wait_send()
        return cc

    lax.fori_loop(0, 8, out_wait, 0)
    for k in range(1, 4):
        zz = (z + k) % 4
        for s in range(2):
            dst = out_ref.at[pl.ds(s * TILE, TILE), pl.ds(pl.multiple_of(zz * width, BLK), width)]
            rc(dst, dst, out_s.at[0], out_r.at[zz, s], me).wait_recv()


def solution(mesh):
    part_size = mesh.shape["part"]
    feat_size = mesh.shape["feat"]

    def local_steps(local_theta, prec_loc, mean_loc, factor_loc):
        rows_loc, feat_loc = local_theta.shape
        n_total = rows_loc * part_size
        feat_total = feat_loc * feat_size
        width = feat_loc // part_size
        kern_width = 2.0 * feat_total / math.log(n_total)
        step_size = 0.15 * n_total * feat_total / math.log(n_total)
        start = lax.axis_index("part") * width
        prec = lax.dynamic_slice_in_dim(prec_loc, start, width)[None, :]
        mean = lax.dynamic_slice_in_dim(mean_loc, start, width)[None, :]
        factor = lax.dynamic_slice_in_dim(factor_loc, start, width)
        rank = factor.shape[1]
        u0 = jnp.pad(factor, ((0, 0), (0, BLK - rank)))
        u1 = jnp.pad(factor, ((0, 0), (BLK - rank, 0)))
        vmem = pl.BlockSpec(memory_space=pltpu.VMEM)
        anym = pl.BlockSpec(memory_space=pl.ANY)
        dma = pltpu.SemaphoreType.DMA
        body = lambda *refs: _kernel(n_total, kern_width, step_size, *refs)
        return pl.pallas_call(
            body,
            out_shape=jax.ShapeDtypeStruct((rows_loc, feat_loc), F32),
            in_specs=[anym, vmem, vmem, vmem, vmem],
            out_specs=anym,
            scratch_shapes=[
                pltpu.VMEM((n_total, width), F32),
                pltpu.VMEM((2, n_total, width), BF),
                pltpu.VMEM((n_total, width), BF),
                pltpu.VMEM((n_total, width), BF),
                pltpu.VMEM((8, BLK, PW), F32),
                pltpu.VMEM((2, BLK, PW), F32),
                pltpu.VMEM((2, 3 * NCH, CH, PW), F32),
                pltpu.VMEM((BLK, PW), F32),
                pltpu.VMEM((2, 8, BLK, PW), BF),
                pltpu.VMEM((2, n_total // 2, n_total), BF),
                pltpu.VMEM((8, BLK // 2, BLK), F32),
                pltpu.VMEM((9, BLK // 2, BLK), F32),
                pltpu.VMEM((9, BLK // 2, BLK), F32),
                pltpu.VMEM((16, BLK), F32),
                dma((4,)), dma((4,)), dma((8,)), dma((8,)), dma, dma,
                dma((2, NCH)), dma((2, NCH)), dma((2, 3 * NCH)), dma((2, 3 * NCH)), dma((NCH,)), dma((NCH,)),
                dma((2, 3 * KCH)), dma((2, 3 * KCH)), dma((2, 2, KCH)), dma((2, 2, KCH)), dma((8, KCH)), dma((8, KCH)),
                dma((8,)), dma((4, 2)),
            ],
            compiler_params=pltpu.CompilerParams(collective_id=0, has_side_effects=True, vmem_limit_bytes=63 * 1024 * 1024),
            name="svgd",
        )(local_theta, prec, mean, u0, u1)

    row_spec = P(("ens", "part"), "feat")
    vec_spec = P(("ens", "feat"))
    fac_spec = P(("ens", "feat"), None)
    return jax.shard_map(local_steps, mesh=mesh, in_specs=(row_spec, vec_spec, vec_spec, fac_spec), out_specs=row_spec, check_vma=False)
```

```python
import math
import jax
import jax.numpy as jnp
from jax import lax
from jax.experimental import pallas as pl
from jax.experimental.pallas import tpu as pltpu
from jax.sharding import PartitionSpec as P

NUM_STEPS = 3
BLK = 128
SPAN = 9
PW = (SPAN + 1) * BLK
GW = SPAN * BLK
NCH = 8
CH = BLK // NCH
KCH = 4
HR = BLK // 2
FSTART = 4
YFWD = (17, 20, 22, 23)
SKEW = 3
TILE = 256
BF = jnp.bfloat16
F32 = jnp.float32
MESH = pl.DeviceIdType.MESH
NT = (((1,), (1,)), ((), ()))


def _dot(a, b):
    return jnp.dot(a, b, preferred_element_type=F32)


def _dot_nt(a, b):
    return lax.dot_general(a, b, NT, preferred_element_type=F32)


def _kernel(n_total, kern_width, step_size,
            theta_in, prec_in, mean_in, fact_in, out_ref,
            th, tb, tsib, ab, gp, fr, cr, zr, kp, k2, zall, zrcv, sfull, prec_ref, mean_ref, u0_ref, u1_ref, par_s,
            in_s, in_r, tx_s, tx_r, zx_s, zx_r, fy_s, fy_r, ch_s, ch_r, zy_s, zy_r,
            kc_s, kc_r, ky_s, ky_r, kx_s, kx_r, out_s, out_r):
    z = lax.axis_index("part")
    f = lax.axis_index("feat")
    y = f // 2
    c = f % 2
    width = th.shape[1]
    half = n_total // 2
    group = n_total // 4

    def dev(zz, yy, cc):
        return {"part": zz, "feat": 2 * yy + cc}

    me = dev(z, y, c)
    ynb = dev(z, 1 - y, c)
    sib = dev(z, y, 1 - c)
    is_end = jnp.logical_or(z == 0, z == 3)
    is_mid = jnp.logical_not(is_end)
    e1 = jnp.where(z < 2, 1, 0)
    e2 = 1 - e1

    def toward(e):
        return dev(jnp.clip(z + 2 * e - 1, 0, 3), y, c)

    def away(e):
        return dev(jnp.clip(z - 2 * e + 1, 0, 3), y, c)

    def rc(src, dst, ss, rs, d):
        return pltpu.make_async_remote_copy(src_ref=src, dst_ref=dst, send_sem=ss, recv_sem=rs,
                                            device_id=d, device_id_type=MESH)

    bar = pltpu.get_barrier_semaphore()
    for k in range(1, 4):
        pl.semaphore_signal(bar, inc=1, device_id=dev((z + k) % 4, y, c), device_id_type=MESH)
    pl.semaphore_signal(bar, inc=1, device_id=ynb, device_id_type=MESH)
    pl.semaphore_signal(bar, inc=1, device_id=sib, device_id_type=MESH)
    pl.semaphore_wait(bar, 5)

    mine = pl.ds(pl.multiple_of(z * width, BLK), width)
    rank = fact_in.shape[0]
    pars = (pltpu.make_async_copy(prec_in.at[:, mine], prec_ref, par_s.at[0]),
            pltpu.make_async_copy(mean_in.at[:, mine], mean_ref, par_s.at[1]),
            pltpu.make_async_copy(fact_in.at[:, mine], u0_ref.at[pl.ds(0, rank), :], par_s.at[2]),
            pltpu.make_async_copy(fact_in.at[:, mine], u1_ref.at[pl.ds(HR, rank), :], par_s.at[3]))

    def grp(zz):
        return pl.multiple_of(((zz + 4 - 2 * c) % 4) * group, group)

    def in_copy(zz):
        return rc(theta_in.at[:, pl.ds(pl.multiple_of(zz * width, BLK), width)], th.at[pl.ds(grp(z), group), :],
                  in_s.at[zz], in_r.at[z], dev(zz, y, c))

    def in_local():
        return pltpu.make_async_copy(theta_in.at[:, pl.ds(pl.multiple_of(z * width, BLK), width)],
                                     th.at[pl.ds(grp(z), group), :], in_r.at[z])

    in_local().start()
    for dist in (3, 2, 1):
        for zz in (z + dist, z - dist):
            @pl.when(jnp.logical_and(zz >= 0, zz < 4))
            def _(zz=zz):
                in_copy(zz).start()

    for p in pars:
        p.start()
    u0_ref[HR:BLK, :] = jnp.zeros((HR, width), BF)
    u1_ref[0:HR, :] = jnp.zeros((HR, width), BF)
    if rank < HR:
        u0_ref[rank:HR, :] = jnp.zeros((HR - rank, width), BF)
        u1_ref[HR + rank:BLK, :] = jnp.zeros((HR - rank, width), BF)
    for p in pars:
        p.wait()

    def t_copy(par, i):
        src = tb.at[par, pl.ds(pl.multiple_of(i * TILE, TILE), TILE), :]
        dst = tsib.at[pl.ds(pl.multiple_of(((i + 4) % 8) * TILE, TILE), TILE), :]
        return rc(src, dst, tx_s.at[i], tx_r.at[(i + 4) % 8], sib)

    def z_copy():
        return rc(zall.at[pl.ds(8, 9)], zrcv, zx_s, zx_r, sib)

    eye = (lax.broadcasted_iota(jnp.int32, (BLK, BLK), 0) == lax.broadcasted_iota(jnp.int32, (BLK, BLK), 1))

    def finish_rows(i, par):
        rows = pl.ds(pl.multiple_of(i * TILE, TILE), TILE)
        tt = th[rows, :].astype(BF)
        tb[par, rows, :] = tt
        z_tile = _dot_nt((th[rows, :] - mean_ref[...]).astype(BF), u0_ref[...])
        low_lanes = lax.broadcasted_iota(jnp.int32, (HR, BLK), 1) < HR
        for s in range(TILE // BLK):
            b = i * (TILE // BLK) + s
            t_blk = tt[s * BLK:(s + 1) * BLK].astype(F32)
            s_col = jnp.sum(t_blk * t_blk, axis=1, keepdims=True)
            s_row = jnp.sum(jnp.where(eye, jnp.broadcast_to(s_col, (BLK, BLK)), 0.0), axis=0, keepdims=True)
            zall[16, pl.ds(b, 1), :] = s_row
            z_blk = z_tile[s * BLK:(s + 1) * BLK]
            zall[b] = jnp.where(low_lanes, z_blk[:HR], pltpu.roll(z_blk[HR:], HR, 1))

    def first_rows(k, carry):
        zz = (z + k) % 4

        @pl.when(k == 0)
        def _():
            in_local().wait()

        @pl.when(k > 0)
        def _():
            rc(th.at[pl.ds(grp(zz), group), :], th.at[pl.ds(grp(zz), group), :], in_s.at[zz], in_r.at[zz], me).wait_recv()
        for s in range(group // TILE):
            i = ((zz + 4 - 2 * c) % 4) * (group // TILE) + s
            finish_rows(i, 0)
            t_copy(0, i).start()
        return carry

    lax.fori_loop(0, 4, first_rows, 0)
    z_copy().start()
    for k in range(1, 4):
        in_copy((z + k) % 4).wait_send()

    def qf(yy, e):
        return yy * 2 + e

    def qz(yy, e):
        return 4 + yy * 2 + e

    def crow(i):
        return pl.ds(i * CH, CH)

    def fy_copy(e, i):
        return rc(gp.at[qf(1 - y, e), crow(i), :], fr.at[e, crow(i), :], fy_s.at[e, i], fy_r.at[e, i], ynb)

    def chain_q(n, e):
        return (qz(1 - y, e), qz(y, e), qf(y, e))[n // NCH]

    def chain_copy(n, e):
        return rc(gp.at[chain_q(n, e), crow(n % NCH), :], cr.at[e, n], ch_s.at[e, n], ch_r.at[e, n], toward(e))

    def zy_copy(i):
        return rc(gp.at[qz(1 - y, e2), crow(i), :], zr.at[crow(i), :], zy_s.at[i], zy_r.at[i], ynb)

    def krow(ch):
        return pl.ds(ch * (BLK // KCH), BLK // KCH)

    def kc_copy(e, j, ch, q):
        return rc(kp.at[0, q, krow(ch), :], kp.at[0, q, krow(ch), :], kc_s.at[e, j * KCH + ch], kc_r.at[e, j * KCH + ch], away(e))

    def ky_copy(e, kind, ch, q):
        return rc(kp.at[0, q, krow(ch), :], kp.at[0, q, krow(ch), :], ky_s.at[e, kind, ch], ky_r.at[e, kind, ch], ynb)

    def kx_copy(ch, q):
        return rc(kp.at[0, q, krow(ch), :], kp.at[1, q, krow(ch), :], kx_s.at[q, ch], kx_r.at[q, ch], sib)

    def step(t, carry):
        par = t % 2

        def t_wait(i, cc):
            t_copy(par, i).wait()
            return cc

        lax.fori_loop(0, 8, t_wait, 0)
        z_copy().wait()
        sfull[0:8, :] = zall[16, 0:8, :] + zrcv[8, 8:16, :]
        sfull[8:16, :] = zall[16, 8:16, :] + zrcv[8, 0:8, :]

        def panel(q):
            rows = pl.ds(pl.multiple_of(q * BLK, BLK), BLK)
            win = pl.ds(pl.multiple_of(q * BLK, BLK), GW)
            gp[q, :, 0:GW] = _dot_nt(tb[par, rows, :], tb[par, win, :]) + _dot_nt(tsib[rows, :], tsib[win, :])
            gp[q, 0:16, GW:PW] = sfull[...]
            gp[q, 16:80, GW:PW] = zall[q] + zrcv[q]
            gp[q, 80:BLK, GW:PW] = jnp.zeros((BLK - 80, BLK), F32)

        def mk_panels(m, cc):
            k = jnp.where(is_end, jnp.where(m == 0, 2, jnp.where(m < 3, m - 1, 3)), m)
            e = jnp.where(k % 2 == 0, e1, e2)
            panel(jnp.where(k < 2, qf(1 - y, e), qz(1 - y, e)))

            @pl.when(jnp.logical_and(k < 2, jnp.logical_or(is_mid, k == 0)))
            def _():
                for i in range(NCH):
                    fy_copy(e, i).start()

            @pl.when(jnp.logical_and(is_end, m == 0))
            def _():
                for i in range(NCH):
                    chain_copy(i, e1).start()
            return cc

        lax.fori_loop(0, 4, mk_panels, 0)

        def late_panels(m, cc):
            e = jnp.where(m % 2 == 0, e1, e2)
            panel(jnp.where(m < 2, qz(y, e), qf(y, e)))

            @pl.when(jnp.logical_and(is_end, m == 0))
            def _():
                for i in range(NCH):
                    chain_copy(NCH + i, e1).start()
            return cc

        KR = BLK // KCH

        def kern_chunk(q, ch):
            rows = slice(ch * KR, (ch + 1) * KR)
            diag = lax.broadcasted_iota(jnp.int32, (KR, BLK), 0) + ch * KR == lax.broadcasted_iota(jnp.int32, (KR, BLK), 1)
            s_col = jnp.sum(jnp.where(diag, jnp.broadcast_to(sfull[pl.ds(q, 1), :], (KR, BLK)), 0.0), axis=1, keepdims=True)
            for k in range(SPAN):
                cols = slice(k * BLK, (k + 1) * BLK)
                dist = jnp.maximum(s_col + sfull[pl.ds(q + k, 1), :] - 2.0 * gp[q, rows, cols], 0.0)
                kp[0, q, rows, cols] = jnp.exp(dist * (-1.0 / kern_width)).astype(BF)
            if ch < KCH // 2:
                kp[0, q, rows, GW:PW] = jnp.zeros((KR, BLK), BF)
            else:
                zr0 = 16 + (ch - KCH // 2) * KR
                kp[0, q, rows, GW:PW] = gp[q, zr0:zr0 + KR, GW:PW].astype(BF)

        def send_own(j, q, ch):
            kern_chunk(q, ch)
            kc_copy(e2, j, ch, q).start()
            ky_copy(e2, 1 if j == 0 else 0, ch, q).start()
            kx_copy(ch, q).start()

        def take(n, e, with_chain, with_y):
            i = n % NCH
            rows = crow(i)
            q = chain_q(n, e)
            val = gp[q, rows, :]
            if with_y:
                rc(fr.at[e, rows, :], fr.at[e, rows, :], fy_s.at[e, i], fy_r.at[e, i], me).wait_recv()
                val = val + fr[e, rows, :]
            if with_chain:
                rc(cr.at[e, n], cr.at[e, n], ch_s.at[e, n], ch_r.at[e, n], me).wait_recv()
                val = val + cr[e, n]
            gp[q, rows, :] = val

        def panel_q(j, e):
            return jnp.where(j == 0, qz(y, e), jnp.where(j == 1, qf(y, e), qz(1 - y, e)))

        def k_take(m, e, fwd):
            j, ch = m // KCH, m % KCH
            q = panel_q(j, e)
            rows = pl.ds(pl.multiple_of(ch * (BLK // KCH), BLK // KCH), BLK // KCH)
            buf = kp.at[0, q, rows, :]
            rc(buf, buf, kc_s.at[e, m], kc_r.at[e, m], me).wait_recv()
            if fwd:
                rc(buf, buf, kc_s.at[e, m], kc_r.at[e, m], away(e)).start()

            @pl.when(j == 1)
            def _():
                rc(buf, buf, ky_s.at[e, 0, ch], ky_r.at[e, 0, ch], ynb).start()
            rc(buf, kp.at[1, q, rows, :], kx_s.at[q, ch], kx_r.at[q, ch], sib).start()

        def mid_round(m):
            for n, e in ((m, e1), (m - SKEW, e2)):
                if 0 <= n < 3 * NCH:
                    take(n, e, True, n >= 2 * NCH)
                    chain_copy(n, e).start()
                elif n >= 3 * NCH:
                    k_take(jnp.int32(n - 3 * NCH), e2, True)

        def end_round(n):
            if FSTART <= n < FSTART + NCH // 2:
                for k in range(2):
                    nn = 2 * NCH + 2 * (n - FSTART) + k
                    take(nn, e1, False, True)
                    chain_copy(nn, e1).start()
            take(n, e2, True, n >= 2 * NCH)
            if n < NCH:
                zy_copy(n).start()
            if NCH <= n < 2 * NCH:
                i = n - NCH
                rows = crow(i)
                rc(zr.at[rows, :], zr.at[rows, :], zy_s.at[i], zy_r.at[i], me).wait_recv()
                q = qz(y, e2)
                gp[q, rows, :] = gp[q, rows, :] + zr[rows, :]
                if n == NCH:
                    sfull[...] = gp[q, 0:16, GW:PW]
            if NCH - 1 <= n < 2 * NCH - 1:
                fy_copy(e2, n - NCH + 1).start()
            per = NCH // KCH
            if n >= NCH and n % per == per - 1:
                if n < 2 * NCH:
                    send_own(0, qz(y, e2), (n - NCH) // per)
                else:
                    send_own(1, qf(y, e2), (n - 2 * NCH) // per)
            if n in YFWD:
                ch = YFWD.index(n)
                q = qz(1 - y, e2)
                buf = kp.at[0, q, krow(ch), :]
                rc(buf, buf, ky_s.at[e2, 1, ch], ky_r.at[e2, 1, ch], me).wait_recv()
                kc_copy(e2, 2, ch, q).start()
                kx_copy(ch, q).start()

        @pl.when(is_mid)
        def _():
            for m in range(3 * NCH + SKEW):
                if m < 4:
                    lax.fori_loop(m, m + 1, late_panels, 0)
                mid_round(m)

        @pl.when(is_end)
        def _():
            lax.fori_loop(0, 4, late_panels, 0)
            for n in range(3 * NCH):
                end_round(n)

        def assemble(h, q):
            lo = pl.ds(pl.multiple_of(q * BLK, BLK), BLK)
            for k in range(SPAN):
                blk = kp[h, q, :, k * BLK:(k + 1) * BLK]
                k2[h, lo, pl.ds(pl.multiple_of((q + k) * BLK, BLK), BLK)] = blk
                if 1 <= k <= 7:
                    flip = (q + k) // 8
                    k2[(h + flip) % 2, pl.ds(pl.multiple_of((q + k - 8 * flip) * BLK, BLK), BLK),
                       pl.ds(pl.multiple_of((q + 8 * flip) * BLK, BLK), BLK)] = blk.T
            zb = kp[h, q, HR:BLK, GW:PW]
            for s, u_ref in ((0, u0_ref), (1, u1_ref)):
                rows = pl.ds(pl.multiple_of((h * 8 + q) * BLK + s * HR, HR), HR)
                low = _dot(zb, u_ref[...])
                x_dev = th[rows, :] - mean_ref[...]
                ab[rows, :] = (-(x_dev * prec_ref[...] + low)).astype(BF)

        def from_sib(q):
            for ch in range(KCH):
                buf = kp.at[1, q, krow(ch), :]
                rc(buf, buf, kx_s.at[q, ch], kx_r.at[q, ch], me).wait_recv()
            assemble(1, q)

        def from_y(e):
            q = qf(1 - y, e)
            for ch in range(KCH):
                buf = kp.at[0, q, krow(ch), :]
                rc(buf, buf, ky_s.at[e, 0, ch], ky_r.at[e, 0, ch], me).wait_recv()
                kx_copy(ch, q).start()
            assemble(0, q)

        def k_round(m, cc):
            near = m + SKEW < 3 * KCH
            nn = jnp.minimum(m + SKEW, 3 * KCH - 1)

            @pl.when(jnp.logical_and(near, is_mid))
            def _():
                k_take(nn, e2, True)

            @pl.when(is_mid)
            def _():
                k_take(m, e1, True)

            @pl.when(is_end)
            def _():
                k_take(m, e1, False)

            @pl.when(jnp.logical_and(near, nn % KCH == KCH - 1))
            def _():
                assemble(0, panel_q(nn // KCH, e2))

            @pl.when(jnp.logical_and(near, jnp.logical_and(nn % KCH == KCH - 1, nn >= KCH)))
            def _():
                from_sib(panel_q(nn // KCH - 1, e2))

            @pl.when(m % KCH == KCH - 1)
            def _():
                assemble(0, panel_q(m // KCH, e1))

            @pl.when(jnp.logical_and(m % KCH == KCH - 1, m >= KCH))
            def _():
                from_sib(panel_q(m // KCH - 1, e1))
            return cc

        lax.fori_loop(0, 3 * KCH, k_round, 0)
        from_y(e2)
        from_y(e1)

        def last_sib(k, cc):
            from_sib(jnp.where(k == 0, qf(1 - y, e2), jnp.where(k == 1, qf(1 - y, e1), jnp.where(k == 2, panel_q(2, e2), panel_q(2, e1)))))
            return cc

        lax.fori_loop(0, 4, last_sib, 0)

        for e in range(2):
            for i in range(NCH):
                fy_copy(e, i).wait_send()
        for n in range(3 * NCH):
            chain_copy(n, e1).wait_send()

            @pl.when(is_mid)
            def _(n=n):
                chain_copy(n, e2).wait_send()

        @pl.when(is_end)
        def _():
            for i in range(NCH):
                zy_copy(i).wait_send()

        def tile_of(k):
            low = z < 2
            zm = jnp.where(low, z, 3 - z)
            zo = jnp.where(k < 2, 2, jnp.where(k < 4, 3, jnp.where(k < 6, 1 - zm, zm)))
            zz = jnp.where(low, zo, 3 - zo)
            return zz, ((zz + 4 - 2 * c) % 4) * 2 + k % 2

        def phi_tile(k, cc):
            zz, i = tile_of(k)
            _, done = tile_of(jnp.maximum(k - 1, 0))
            finish_rows(done, 1 - par)
            h = i // 4
            rows = pl.ds(pl.multiple_of(i * TILE, TILE), TILE)
            krows = pl.ds(pl.multiple_of((i % 4) * TILE, TILE), TILE)
            first = pl.ds(pl.multiple_of(h * half, half), half)
            second = pl.ds(pl.multiple_of((1 - h) * half, half), half)
            ka = k2[h, krows, 0:half]
            kb = k2[h, krows, half:n_total]
            drive = _dot(ka, ab[first, :]) + _dot(kb, ab[second, :])
            pull = _dot(ka, tb[par, first, :]) + _dot(kb, tb[par, second, :])
            mass = jnp.sum(ka.astype(F32), axis=1, keepdims=True) + jnp.sum(kb.astype(F32), axis=1, keepdims=True)
            t_own = tb[par, rows, :].astype(F32)
            upd = (drive + (2.0 / kern_width) * (mass * t_own - pull)) * (1.0 / n_total)
            th[rows, :] = th[rows, :] + step_size * upd

            @pl.when(jnp.logical_and(t < NUM_STEPS - 1, k > 0))
            def _():
                t_copy(1 - par, done).start()

            @pl.when(t == NUM_STEPS - 1)
            def _():
                dst = out_ref.at[pl.ds(pl.multiple_of((i % 2) * TILE, TILE), TILE), pl.ds(pl.multiple_of(z * width, BLK), width)]

                @pl.when(zz == z)
                def _():
                    pltpu.make_async_copy(th.at[rows, :], dst, out_s.at[i]).start()

                @pl.when(zz != z)
                def _():
                    rc(th.at[rows, :], dst, out_s.at[i], out_r.at[z, i % 2], dev(zz, y, c)).start()
            return cc

        lax.fori_loop(0, 8, phi_tile, 0)

        @pl.when(t < NUM_STEPS - 1)
        def _():
            _, done = tile_of(7)
            finish_rows(done, 1 - par)
            t_copy(1 - par, done).start()
            z_copy().start()

        for ch in range(KCH):
            for e in range(2):
                ky_copy(e, 0, ch, qf(y, e)).wait_send()

            @pl.when(is_end)
            def _(ch=ch):
                ky_copy(e2, 1, ch, qz(y, e2)).wait_send()
            for j in range(3):
                q2 = (qz(y, e2), qf(y, e2), qz(1 - y, e2))[j]
                q1 = (qz(y, e1), qf(y, e1), qz(1 - y, e1))[j]
                kc_copy(e2, j, ch, q2).wait_send()

                @pl.when(is_mid)
                def _(ch=ch, j=j, q1=q1):
                    kc_copy(e1, j, ch, q1).wait_send()
            for q in range(8):
                kx_copy(ch, q).wait_send()
        return carry

    lax.fori_loop(0, NUM_STEPS, step, 0)

    def out_wait(i, cc):
        zz = (i // 2 + 2 * c) % 4
        rows = pl.ds(pl.multiple_of(i * TILE, TILE), TILE)
        dst = out_ref.at[pl.ds(pl.multiple_of((i % 2) * TILE, TILE), TILE), pl.ds(pl.multiple_of(z * width, BLK), width)]

        @pl.when(zz == z)
        def _():
            pltpu.make_async_copy(th.at[rows, :], dst, out_s.at[i]).wait()

        @pl.when(zz != z)
        def _():
            rc(th.at[rows, :], dst, out_s.at[i], out_r.at[z, i % 2], dev(zz, y, c)).wait_send()
        return cc

    lax.fori_loop(0, 8, out_wait, 0)
    for k in range(1, 4):
        zz = (z + k) % 4
        for s in range(2):
            dst = out_ref.at[pl.ds(s * TILE, TILE), pl.ds(pl.multiple_of(zz * width, BLK), width)]
            rc(dst, dst, out_s.at[0], out_r.at[zz, s], me).wait_recv()


def solution(mesh):
    part_size = mesh.shape["part"]
    feat_size = mesh.shape["feat"]

    def local_steps(local_theta, prec_loc, mean_loc, factor_loc):
        rows_loc, feat_loc = local_theta.shape
        n_total = rows_loc * part_size
        feat_total = feat_loc * feat_size
        width = feat_loc // part_size
        kern_width = 2.0 * feat_total / math.log(n_total)
        step_size = 0.15 * n_total * feat_total / math.log(n_total)
        anym = pl.BlockSpec(memory_space=pl.ANY)
        dma = pltpu.SemaphoreType.DMA
        body = lambda *refs: _kernel(n_total, kern_width, step_size, *refs)
        return pl.pallas_call(
            body,
            out_shape=jax.ShapeDtypeStruct((rows_loc, feat_loc), F32),
            in_specs=[anym, anym, anym, anym],
            out_specs=anym,
            scratch_shapes=[
                pltpu.VMEM((n_total, width), F32),
                pltpu.VMEM((2, n_total, width), BF),
                pltpu.VMEM((n_total, width), BF),
                pltpu.VMEM((n_total, width), BF),
                pltpu.VMEM((8, BLK, PW), F32),
                pltpu.VMEM((2, BLK, PW), F32),
                pltpu.VMEM((2, 3 * NCH, CH, PW), F32),
                pltpu.VMEM((BLK, PW), F32),
                pltpu.VMEM((2, 8, BLK, PW), BF),
                pltpu.VMEM((2, n_total // 2, n_total), BF),
                pltpu.VMEM((17, HR, BLK), F32),
                pltpu.VMEM((9, HR, BLK), F32),
                pltpu.VMEM((16, BLK), F32),
                pltpu.VMEM((1, width), F32), pltpu.VMEM((1, width), F32),
                pltpu.VMEM((BLK, width), BF), pltpu.VMEM((BLK, width), BF),
                dma((4,)),
                dma((4,)), dma((4,)), dma((8,)), dma((8,)), dma, dma,
                dma((2, NCH)), dma((2, NCH)), dma((2, 3 * NCH)), dma((2, 3 * NCH)), dma((NCH,)), dma((NCH,)),
                dma((2, 3 * KCH)), dma((2, 3 * KCH)), dma((2, 2, KCH)), dma((2, 2, KCH)), dma((8, KCH)), dma((8, KCH)),
                dma((8,)), dma((4, 2)),
            ],
            compiler_params=pltpu.CompilerParams(collective_id=0, has_side_effects=True, vmem_limit_bytes=63 * 1024 * 1024),
            name="svgd",
        )(local_theta, prec_loc[None, :], mean_loc[None, :], factor_loc.T)

    row_spec = P(("ens", "part"), "feat")
    vec_spec = P(("ens", "feat"))
    fac_spec = P(("ens", "feat"), None)
    return jax.shard_map(local_steps, mesh=mesh, in_specs=(row_spec, vec_spec, vec_spec, fac_spec), out_specs=row_spec, check_vma=False)
```

```python
import math
import jax
import jax.numpy as jnp
from jax import lax
from jax.experimental import pallas as pl
from jax.experimental.pallas import tpu as pltpu
from jax.sharding import PartitionSpec as P

NUM_STEPS = 3
BLK = 128
SPAN = 8
PW = (SPAN + 1) * BLK
GW = SPAN * BLK
NCH = 8
CH = BLK // NCH
KCH = 4
HR = BLK // 2
FSTART = 4
YFWD = (17, 20, 22, 23)
SKEW = 3
TILE = 256
BF = jnp.bfloat16
F32 = jnp.float32
MESH = pl.DeviceIdType.MESH
NT = (((1,), (1,)), ((), ()))


def _dot(a, b):
    return jnp.dot(a, b, preferred_element_type=F32)


def _dot_nt(a, b):
    return lax.dot_general(a, b, NT, preferred_element_type=F32)


def _kernel(n_total, kern_width, step_size,
            theta_in, prec_in, mean_in, fact_in, out_ref,
            th, tb, tsib, ab, gp, fr, cr, zr, kp, k2, zall, zrcv, sfull, sown, sbuf, prec_ref, mean_ref, u0_ref, u1_ref, par_s, sx_s, sx_r,
            in_s, in_r, tx_s, tx_r, zx_s, zx_r, fy_s, fy_r, ch_s, ch_r, zy_s, zy_r,
            kc_s, kc_r, ky_s, ky_r, kx_s, kx_r, out_s, out_r):
    z = lax.axis_index("part")
    f = lax.axis_index("feat")
    y = f // 2
    c = f % 2
    width = th.shape[1]
    half = n_total // 2
    group = n_total // 4

    def dev(zz, yy, cc):
        return {"part": zz, "feat": 2 * yy + cc}

    me = dev(z, y, c)
    ynb = dev(z, 1 - y, c)
    sib = dev(z, y, 1 - c)
    is_end = jnp.logical_or(z == 0, z == 3)
    is_mid = jnp.logical_not(is_end)
    e1 = jnp.where(z < 2, 1, 0)
    e2 = 1 - e1

    def toward(e):
        return dev(jnp.clip(z + 2 * e - 1, 0, 3), y, c)

    def away(e):
        return dev(jnp.clip(z - 2 * e + 1, 0, 3), y, c)

    def rc(src, dst, ss, rs, d):
        return pltpu.make_async_remote_copy(src_ref=src, dst_ref=dst, send_sem=ss, recv_sem=rs,
                                            device_id=d, device_id_type=MESH)

    bar = pltpu.get_barrier_semaphore()
    for k in range(1, 4):
        pl.semaphore_signal(bar, inc=1, device_id=dev((z + k) % 4, y, c), device_id_type=MESH)
    for k in range(4):
        pl.semaphore_signal(bar, inc=1, device_id=dev((z + k) % 4, 1 - y, c), device_id_type=MESH)
    pl.semaphore_signal(bar, inc=1, device_id=sib, device_id_type=MESH)
    pl.semaphore_wait(bar, 8)

    mine = pl.ds(pl.multiple_of(z * width, BLK), width)
    rank = fact_in.shape[0]
    pars = (pltpu.make_async_copy(prec_in.at[:, mine], prec_ref, par_s.at[0]),
            pltpu.make_async_copy(mean_in.at[:, mine], mean_ref, par_s.at[1]),
            pltpu.make_async_copy(fact_in.at[:, mine], u0_ref.at[pl.ds(0, rank), :], par_s.at[2]),
            pltpu.make_async_copy(fact_in.at[:, mine], u1_ref.at[pl.ds(HR, rank), :], par_s.at[3]))

    def grp(zz):
        return pl.multiple_of(((zz + 4 - 2 * c) % 4) * group, group)

    def in_copy(zz):
        return rc(theta_in.at[:, pl.ds(pl.multiple_of(zz * width, BLK), width)], th.at[pl.ds(grp(z), group), :],
                  in_s.at[zz], in_r.at[z], dev(zz, y, c))

    def in_local():
        return pltpu.make_async_copy(theta_in.at[:, pl.ds(pl.multiple_of(z * width, BLK), width)],
                                     th.at[pl.ds(grp(z), group), :], in_r.at[z])

    in_local().start()
    for dist in (3, 2, 1):
        for zz in (z + dist, z - dist):
            @pl.when(jnp.logical_and(zz >= 0, zz < 4))
            def _(zz=zz):
                in_copy(zz).start()

    for p in pars:
        p.start()
    u0_ref[HR:BLK, :] = jnp.zeros((HR, width), BF)
    u1_ref[0:HR, :] = jnp.zeros((HR, width), BF)
    if rank < HR:
        u0_ref[rank:HR, :] = jnp.zeros((HR - rank, width), BF)
        u1_ref[HR + rank:BLK, :] = jnp.zeros((HR - rank, width), BF)
    for p in pars:
        p.wait()

    def t_copy(par, i):
        src = tb.at[par, pl.ds(pl.multiple_of(i * TILE, TILE), TILE), :]
        dst = tsib.at[pl.ds(pl.multiple_of(((i + 4) % 8) * TILE, TILE), TILE), :]
        return rc(src, dst, tx_s.at[i], tx_r.at[(i + 4) % 8], sib)

    def z_copy():
        return rc(zall.at[pl.ds(8, 9)], zrcv, zx_s, zx_r, sib)

    eye = (lax.broadcasted_iota(jnp.int32, (BLK, BLK), 0) == lax.broadcasted_iota(jnp.int32, (BLK, BLK), 1))

    def finish_rows(i, par):
        rows = pl.ds(pl.multiple_of(i * TILE, TILE), TILE)
        tt = th[rows, :].astype(BF)
        tb[par, rows, :] = tt
        z_tile = _dot_nt((th[rows, :] - mean_ref[...]).astype(BF), u0_ref[...])
        low_lanes = lax.broadcasted_iota(jnp.int32, (HR, BLK), 1) < HR
        for s in range(TILE // BLK):
            b = i * (TILE // BLK) + s
            t_blk = tt[s * BLK:(s + 1) * BLK].astype(F32)
            s_col = jnp.sum(t_blk * t_blk, axis=1, keepdims=True)
            s_row = jnp.sum(jnp.where(eye, jnp.broadcast_to(s_col, (BLK, BLK)), 0.0), axis=0, keepdims=True)
            zall[16, pl.ds(b, 1), :] = s_row
            z_blk = z_tile[s * BLK:(s + 1) * BLK]
            zall[b] = jnp.where(low_lanes, z_blk[:HR], pltpu.roll(z_blk[HR:], HR, 1))

    def first_rows(k, carry):
        zz = (z + k) % 4

        @pl.when(k == 0)
        def _():
            in_local().wait()

        @pl.when(k > 0)
        def _():
            rc(th.at[pl.ds(grp(zz), group), :], th.at[pl.ds(grp(zz), group), :], in_s.at[zz], in_r.at[zz], me).wait_recv()
        for s in range(group // TILE):
            i = ((zz + 4 - 2 * c) % 4) * (group // TILE) + s
            finish_rows(i, 0)
            t_copy(0, i).start()
        return carry

    lax.fori_loop(0, 4, first_rows, 0)
    z_copy().start()
    for k in range(1, 4):
        in_copy((z + k) % 4).wait_send()

    def qf(yy, e):
        return yy * 2 + e

    def qz(yy, e):
        return 4 + yy * 2 + e

    def crow(i):
        return pl.ds(i * CH, CH)

    def fy_copy(e, i):
        return rc(gp.at[qf(1 - y, e), crow(i), :], fr.at[e, crow(i), :], fy_s.at[e, i], fy_r.at[e, i], ynb)

    def s_copy(yy, e, k):
        return rc(sown, sbuf.at[2 * z + y], sx_s.at[k], sx_r.at[2 * z + y], dev(3 * e, yy, c))

    def chain_q(n, e):
        return (qz(1 - y, e), qz(y, e), qf(y, e))[n // NCH]

    def chain_copy(n, e):
        return rc(gp.at[chain_q(n, e), crow(n % NCH), :], cr.at[e, n], ch_s.at[e, n], ch_r.at[e, n], toward(e))

    def zy_copy(i):
        return rc(gp.at[qz(1 - y, e2), crow(i), :], zr.at[crow(i), :], zy_s.at[i], zy_r.at[i], ynb)

    def krow(ch):
        return pl.ds(ch * (BLK // KCH), BLK // KCH)

    def kc_copy(e, j, ch, q):
        return rc(kp.at[0, q, krow(ch), :], kp.at[0, q, krow(ch), :], kc_s.at[e, j * KCH + ch], kc_r.at[e, j * KCH + ch], away(e))

    def ky_copy(e, kind, ch, q):
        return rc(kp.at[0, q, krow(ch), :], kp.at[0, q, krow(ch), :], ky_s.at[e, kind, ch], ky_r.at[e, kind, ch], ynb)

    def kx_copy(ch, q):
        return rc(kp.at[0, q, krow(ch), :], kp.at[1, q, krow(ch), :], kx_s.at[q, ch], kx_r.at[q, ch], sib)

    def step(t, carry):
        par = t % 2

        def t_wait(i, cc):
            t_copy(par, i).wait()
            return cc

        lax.fori_loop(0, 8, t_wait, 0)
        z_copy().wait()
        sown[0:8, :] = zall[16, 0:8, :] + zrcv[8, 8:16, :]
        sown[8:16, :] = zall[16, 8:16, :] + zrcv[8, 0:8, :]
        for e in range(2):
            s_copy(1 - y, e, 2 + e).start()

            @pl.when(z != 3 * e)
            def _(e=e):
                s_copy(y, e, e).start()

        def panel(q):
            rows = pl.ds(pl.multiple_of(q * BLK, BLK), BLK)
            win = pl.ds(pl.multiple_of(q * BLK, BLK), PW)
            gram = _dot_nt(tb[par, rows, :], tb[par, win, :]) + _dot_nt(tsib[rows, :], tsib[win, :])
            gp[q, :, 0:GW] = gram[:, 0:GW]
            last = gram[:, GW:PW]
            right = jnp.logical_and(c == 1, lax.broadcasted_iota(jnp.int32, (HR, BLK), 1) < HR)
            gp[q, 0:HR, GW:PW] = jnp.where(right, pltpu.roll(last[HR:], HR, 1), last[:HR])
            gp[q, HR:BLK, GW:PW] = zall[q] + zrcv[q]

        def mk_panels(m, cc):
            k = jnp.where(is_end, jnp.where(m == 0, 2, jnp.where(m < 3, m - 1, 3)), m)
            e = jnp.where(k % 2 == 0, e1, e2)
            panel(jnp.where(k < 2, qf(1 - y, e), qz(1 - y, e)))

            @pl.when(jnp.logical_and(k < 2, jnp.logical_or(is_mid, k == 0)))
            def _():
                for i in range(NCH):
                    fy_copy(e, i).start()

            @pl.when(jnp.logical_and(is_end, m == 0))
            def _():
                for i in range(NCH):
                    chain_copy(i, e1).start()
            return cc

        lax.fori_loop(0, 4, mk_panels, 0)

        def late_panels(m, cc):
            e = jnp.where(m % 2 == 0, e1, e2)
            panel(jnp.where(m < 2, qz(y, e), qf(y, e)))

            @pl.when(jnp.logical_and(is_end, m == 0))
            def _():
                for i in range(NCH):
                    chain_copy(NCH + i, e1).start()
            return cc

        KR = BLK // KCH

        def s_column(q, first):
            diag = lax.broadcasted_iota(jnp.int32, (KR, BLK), 0) + first == lax.broadcasted_iota(jnp.int32, (KR, BLK), 1)
            return jnp.sum(jnp.where(diag, jnp.broadcast_to(sfull[pl.ds(q, 1), :], (KR, BLK)), 0.0), axis=1, keepdims=True)

        def kern(s_col, s_row, gram):
            return jnp.exp(jnp.maximum(s_col + s_row - 2.0 * gram, 0.0) * (-1.0 / kern_width)).astype(BF)

        def kern_chunk(q, ch):
            rows = slice(ch * KR, (ch + 1) * KR)
            s_col = s_column(q, ch * KR)
            for k in range(SPAN):
                cols = slice(k * BLK, (k + 1) * BLK)
                kp[0, q, rows, cols] = kern(s_col, sfull[pl.ds(q + k, 1), :], gp[q, rows, cols])
            if ch < KCH // 2:
                right = jnp.logical_and(c == 1, lax.broadcasted_iota(jnp.int32, (KR, BLK), 1) < HR)
                s_row = jnp.broadcast_to(sfull[pl.ds(q + SPAN, 1), :], (KR, BLK))
                kp[0, q, rows, GW:PW] = kern(jnp.where(right, s_column(q, HR + ch * KR), s_col),
                                             jnp.where(right, pltpu.roll(s_row, HR, 1), s_row), gp[q, rows, GW:PW])
            else:
                kp[0, q, rows, GW:PW] = gp[q, rows, GW:PW].astype(BF)

        def send_own(j, q, ch):
            kern_chunk(q, ch)
            kc_copy(e2, j, ch, q).start()
            ky_copy(e2, 1 if j == 0 else 0, ch, q).start()
            kx_copy(ch, q).start()

        def take(n, e, with_chain, with_y):
            i = n % NCH
            rows = crow(i)
            q = chain_q(n, e)
            val = gp[q, rows, :]
            if with_y:
                rc(fr.at[e, rows, :], fr.at[e, rows, :], fy_s.at[e, i], fy_r.at[e, i], me).wait_recv()
                val = val + fr[e, rows, :]
            if with_chain:
                rc(cr.at[e, n], cr.at[e, n], ch_s.at[e, n], ch_r.at[e, n], me).wait_recv()
                val = val + cr[e, n]
            gp[q, rows, :] = val

        def panel_q(j, e):
            return jnp.where(j == 0, qz(y, e), jnp.where(j == 1, qf(y, e), qz(1 - y, e)))

        def k_take(m, e, fwd):
            j, ch = m // KCH, m % KCH
            q = panel_q(j, e)
            rows = pl.ds(pl.multiple_of(ch * (BLK // KCH), BLK // KCH), BLK // KCH)
            buf = kp.at[0, q, rows, :]
            rc(buf, buf, kc_s.at[e, m], kc_r.at[e, m], me).wait_recv()
            if fwd:
                rc(buf, buf, kc_s.at[e, m], kc_r.at[e, m], away(e)).start()

            @pl.when(j == 1)
            def _():
                rc(buf, buf, ky_s.at[e, 0, ch], ky_r.at[e, 0, ch], ynb).start()
            rc(buf, kp.at[1, q, rows, :], kx_s.at[q, ch], kx_r.at[q, ch], sib).start()

        def mid_round(m):
            for n, e in ((m, e1), (m - SKEW, e2)):
                if 0 <= n < 3 * NCH:
                    take(n, e, True, n >= 2 * NCH)
                    chain_copy(n, e).start()
                elif n >= 3 * NCH:
                    k_take(jnp.int32(n - 3 * NCH), e2, True)

        def end_round(n):
            if FSTART <= n < FSTART + NCH // 2:
                for k in range(2):
                    nn = 2 * NCH + 2 * (n - FSTART) + k
                    take(nn, e1, False, True)
                    chain_copy(nn, e1).start()
            take(n, e2, True, n >= 2 * NCH)
            if n < NCH:
                zy_copy(n).start()
            if NCH <= n < 2 * NCH:
                i = n - NCH
                rows = crow(i)
                rc(zr.at[rows, :], zr.at[rows, :], zy_s.at[i], zy_r.at[i], me).wait_recv()
                q = qz(y, e2)
                gp[q, rows, :] = gp[q, rows, :] + zr[rows, :]
                if n == NCH:
                    sfull[...] = sown[...]
                    for k in range(8):
                        @pl.when(2 * z + y != k)
                        def _(k=k):
                            rc(sbuf.at[k], sbuf.at[k], sx_s.at[0], sx_r.at[k], me).wait_recv()
                            sfull[...] = sfull[...] + sbuf[k]
            if NCH - 1 <= n < 2 * NCH - 1:
                fy_copy(e2, n - NCH + 1).start()
            per = NCH // KCH
            if n >= NCH and n % per == per - 1:
                if n < 2 * NCH:
                    send_own(0, qz(y, e2), (n - NCH) // per)
                else:
                    send_own(1, qf(y, e2), (n - 2 * NCH) // per)
            if n in YFWD:
                ch = YFWD.index(n)
                q = qz(1 - y, e2)
                buf = kp.at[0, q, krow(ch), :]
                rc(buf, buf, ky_s.at[e2, 1, ch], ky_r.at[e2, 1, ch], me).wait_recv()
                kc_copy(e2, 2, ch, q).start()
                kx_copy(ch, q).start()

        @pl.when(is_mid)
        def _():
            for m in range(3 * NCH + SKEW):
                if m < 4:
                    lax.fori_loop(m, m + 1, late_panels, 0)
                mid_round(m)

        @pl.when(is_end)
        def _():
            lax.fori_loop(0, 4, late_panels, 0)
            for n in range(3 * NCH):
                end_round(n)

        def assemble(h, q):
            lo = pl.ds(pl.multiple_of(q * BLK, BLK), BLK)
            for k in range(SPAN):
                blk = kp[h, q, :, k * BLK:(k + 1) * BLK]
                k2[h, lo, pl.ds(pl.multiple_of((q + k) * BLK, BLK), BLK)] = blk
                if k >= 1:
                    flip = (q + k) // 8
                    k2[(h + flip) % 2, pl.ds(pl.multiple_of((q + k - 8 * flip) * BLK, BLK), BLK),
                       pl.ds(pl.multiple_of((q + 8 * flip) * BLK, BLK), BLK)] = blk.T
            zb = kp[h, q, HR:BLK, GW:PW]
            for s, u_ref in ((0, u0_ref), (1, u1_ref)):
                rows = pl.ds(pl.multiple_of((h * 8 + q) * BLK + s * HR, HR), HR)
                low = _dot(zb, u_ref[...])
                x_dev = th[rows, :] - mean_ref[...]
                ab[rows, :] = (-(x_dev * prec_ref[...] + low)).astype(BF)

        def pair_block(q):
            upper = kp[c, q, 0:HR, GW:PW].astype(F32)
            right = kp[1 - c, q, 0:HR, GW:PW].astype(F32)
            lower = jnp.concatenate([right, pltpu.roll(right, HR, 1)], axis=0).T[HR:BLK]
            blk = jnp.concatenate([upper, lower], axis=0)
            rows = pl.ds(pl.multiple_of(q * BLK, BLK), BLK)
            cols = pl.ds(pl.multiple_of((q + SPAN) * BLK, BLK), BLK)
            k2[c, rows, cols] = blk.astype(BF)
            k2[1 - c, rows, cols] = blk.T.astype(BF)

        def from_sib(q):
            for ch in range(KCH):
                buf = kp.at[1, q, krow(ch), :]
                rc(buf, buf, kx_s.at[q, ch], kx_r.at[q, ch], me).wait_recv()
            assemble(1, q)
            pair_block(q)

        def from_y(e):
            q = qf(1 - y, e)
            for ch in range(KCH):
                buf = kp.at[0, q, krow(ch), :]
                rc(buf, buf, ky_s.at[e, 0, ch], ky_r.at[e, 0, ch], me).wait_recv()
                kx_copy(ch, q).start()
            assemble(0, q)

        def k_round(m, cc):
            near = m + SKEW < 3 * KCH
            nn = jnp.minimum(m + SKEW, 3 * KCH - 1)

            @pl.when(jnp.logical_and(near, is_mid))
            def _():
                k_take(nn, e2, True)

            @pl.when(is_mid)
            def _():
                k_take(m, e1, True)

            @pl.when(is_end)
            def _():
                k_take(m, e1, False)

            @pl.when(jnp.logical_and(near, nn % KCH == KCH - 1))
            def _():
                assemble(0, panel_q(nn // KCH, e2))

            @pl.when(jnp.logical_and(near, jnp.logical_and(nn % KCH == KCH - 1, nn >= KCH)))
            def _():
                from_sib(panel_q(nn // KCH - 1, e2))

            @pl.when(m % KCH == KCH - 1)
            def _():
                assemble(0, panel_q(m // KCH, e1))

            @pl.when(jnp.logical_and(m % KCH == KCH - 1, m >= KCH))
            def _():
                from_sib(panel_q(m // KCH - 1, e1))
            return cc

        lax.fori_loop(0, 3 * KCH, k_round, 0)
        from_y(e2)
        from_y(e1)

        def last_sib(k, cc):
            from_sib(jnp.where(k == 0, qf(1 - y, e2), jnp.where(k == 1, qf(1 - y, e1), jnp.where(k == 2, panel_q(2, e2), panel_q(2, e1)))))
            return cc

        lax.fori_loop(0, 4, last_sib, 0)

        for e in range(2):
            s_copy(1 - y, e, 2 + e).wait_send()

            @pl.when(z != 3 * e)
            def _(e=e):
                s_copy(y, e, e).wait_send()
            for i in range(NCH):
                fy_copy(e, i).wait_send()
        for n in range(3 * NCH):
            chain_copy(n, e1).wait_send()

            @pl.when(is_mid)
            def _(n=n):
                chain_copy(n, e2).wait_send()

        @pl.when(is_end)
        def _():
            for i in range(NCH):
                zy_copy(i).wait_send()

        def tile_of(k):
            low = z < 2
            zm = jnp.where(low, z, 3 - z)
            zo = jnp.where(k < 2, 2, jnp.where(k < 4, 3, jnp.where(k < 6, 1 - zm, zm)))
            zz = jnp.where(low, zo, 3 - zo)
            return zz, ((zz + 4 - 2 * c) % 4) * 2 + k % 2

        def phi_tile(k, cc):
            zz, i = tile_of(k)
            _, done = tile_of(jnp.maximum(k - 1, 0))
            finish_rows(done, 1 - par)
            h = i // 4
            rows = pl.ds(pl.multiple_of(i * TILE, TILE), TILE)
            krows = pl.ds(pl.multiple_of((i % 4) * TILE, TILE), TILE)
            first = pl.ds(pl.multiple_of(h * half, half), half)
            second = pl.ds(pl.multiple_of((1 - h) * half, half), half)
            ka = k2[h, krows, 0:half]
            kb = k2[h, krows, half:n_total]
            drive = _dot(ka, ab[first, :]) + _dot(kb, ab[second, :])
            pull = _dot(ka, tb[par, first, :]) + _dot(kb, tb[par, second, :])
            mass = jnp.sum(ka.astype(F32), axis=1, keepdims=True) + jnp.sum(kb.astype(F32), axis=1, keepdims=True)
            t_own = tb[par, rows, :].astype(F32)
            upd = (drive + (2.0 / kern_width) * (mass * t_own - pull)) * (1.0 / n_total)
            th[rows, :] = th[rows, :] + step_size * upd

            @pl.when(jnp.logical_and(t < NUM_STEPS - 1, k > 0))
            def _():
                t_copy(1 - par, done).start()

            @pl.when(t == NUM_STEPS - 1)
            def _():
                dst = out_ref.at[pl.ds(pl.multiple_of((i % 2) * TILE, TILE), TILE), pl.ds(pl.multiple_of(z * width, BLK), width)]

                @pl.when(zz == z)
                def _():
                    pltpu.make_async_copy(th.at[rows, :], dst, out_s.at[i]).start()

                @pl.when(zz != z)
                def _():
                    rc(th.at[rows, :], dst, out_s.at[i], out_r.at[z, i % 2], dev(zz, y, c)).start()
            return cc

        lax.fori_loop(0, 8, phi_tile, 0)

        @pl.when(t < NUM_STEPS - 1)
        def _():
            _, done = tile_of(7)
            finish_rows(done, 1 - par)
            t_copy(1 - par, done).start()
            z_copy().start()

        for ch in range(KCH):
            for e in range(2):
                ky_copy(e, 0, ch, qf(y, e)).wait_send()

            @pl.when(is_end)
            def _(ch=ch):
                ky_copy(e2, 1, ch, qz(y, e2)).wait_send()
            for j in range(3):
                q2 = (qz(y, e2), qf(y, e2), qz(1 - y, e2))[j]
                q1 = (qz(y, e1), qf(y, e1), qz(1 - y, e1))[j]
                kc_copy(e2, j, ch, q2).wait_send()

                @pl.when(is_mid)
                def _(ch=ch, j=j, q1=q1):
                    kc_copy(e1, j, ch, q1).wait_send()
            for q in range(8):
                kx_copy(ch, q).wait_send()
        return carry

    lax.fori_loop(0, NUM_STEPS, step, 0)

    def out_wait(i, cc):
        zz = (i // 2 + 2 * c) % 4
        rows = pl.ds(pl.multiple_of(i * TILE, TILE), TILE)
        dst = out_ref.at[pl.ds(pl.multiple_of((i % 2) * TILE, TILE), TILE), pl.ds(pl.multiple_of(z * width, BLK), width)]

        @pl.when(zz == z)
        def _():
            pltpu.make_async_copy(th.at[rows, :], dst, out_s.at[i]).wait()

        @pl.when(zz != z)
        def _():
            rc(th.at[rows, :], dst, out_s.at[i], out_r.at[z, i % 2], dev(zz, y, c)).wait_send()
        return cc

    lax.fori_loop(0, 8, out_wait, 0)
    for k in range(1, 4):
        zz = (z + k) % 4
        for s in range(2):
            dst = out_ref.at[pl.ds(s * TILE, TILE), pl.ds(pl.multiple_of(zz * width, BLK), width)]
            rc(dst, dst, out_s.at[0], out_r.at[zz, s], me).wait_recv()


def solution(mesh):
    part_size = mesh.shape["part"]
    feat_size = mesh.shape["feat"]

    def local_steps(local_theta, prec_loc, mean_loc, factor_loc):
        rows_loc, feat_loc = local_theta.shape
        n_total = rows_loc * part_size
        feat_total = feat_loc * feat_size
        width = feat_loc // part_size
        kern_width = 2.0 * feat_total / math.log(n_total)
        step_size = 0.15 * n_total * feat_total / math.log(n_total)
        anym = pl.BlockSpec(memory_space=pl.ANY)
        dma = pltpu.SemaphoreType.DMA
        body = lambda *refs: _kernel(n_total, kern_width, step_size, *refs)
        return pl.pallas_call(
            body,
            out_shape=jax.ShapeDtypeStruct((rows_loc, feat_loc), F32),
            in_specs=[anym, anym, anym, anym],
            out_specs=anym,
            scratch_shapes=[
                pltpu.VMEM((n_total, width), F32),
                pltpu.VMEM((2, n_total, width), BF),
                pltpu.VMEM((n_total, width), BF),
                pltpu.VMEM((n_total, width), BF),
                pltpu.VMEM((8, BLK, PW), F32),
                pltpu.VMEM((2, BLK, PW), F32),
                pltpu.VMEM((2, 3 * NCH, CH, PW), F32),
                pltpu.VMEM((BLK, PW), F32),
                pltpu.VMEM((2, 8, BLK, PW), BF),
                pltpu.VMEM((2, n_total // 2, n_total), BF),
                pltpu.VMEM((17, HR, BLK), F32),
                pltpu.VMEM((9, HR, BLK), F32),
                pltpu.VMEM((16, BLK), F32), pltpu.VMEM((16, BLK), F32), pltpu.VMEM((8, 16, BLK), F32),
                pltpu.VMEM((1, width), F32), pltpu.VMEM((1, width), F32),
                pltpu.VMEM((BLK, width), BF), pltpu.VMEM((BLK, width), BF),
                dma((4,)), dma((4,)), dma((8,)),
                dma((4,)), dma((4,)), dma((8,)), dma((8,)), dma, dma,
                dma((2, NCH)), dma((2, NCH)), dma((2, 3 * NCH)), dma((2, 3 * NCH)), dma((NCH,)), dma((NCH,)),
                dma((2, 3 * KCH)), dma((2, 3 * KCH)), dma((2, 2, KCH)), dma((2, 2, KCH)), dma((8, KCH)), dma((8, KCH)),
                dma((8,)), dma((4, 2)),
            ],
            compiler_params=pltpu.CompilerParams(collective_id=0, has_side_effects=True, vmem_limit_bytes=63 * 1024 * 1024),
            name="svgd",
        )(local_theta, prec_loc[None, :], mean_loc[None, :], factor_loc.T)

    row_spec = P(("ens", "part"), "feat")
    vec_spec = P(("ens", "feat"))
    fac_spec = P(("ens", "feat"), None)
    return jax.shard_map(local_steps, mesh=mesh, in_specs=(row_spec, vec_spec, vec_spec, fac_spec), out_specs=row_spec, check_vma=False)
```

```python
import math
import jax
import jax.numpy as jnp
from jax import lax
from jax.experimental import pallas as pl
from jax.experimental.pallas import tpu as pltpu
from jax.sharding import PartitionSpec as P

NUM_STEPS = 3
BLK = 128
SPAN = 8
PW = (SPAN + 1) * BLK
GW = SPAN * BLK
NCH = 8
CH = BLK // NCH
KCH = 4
HR = BLK // 2
FSTART = 4
YFWD = (17, 20, 22, 23)
SKEW = 3
TILE = 256
BF = jnp.bfloat16
F32 = jnp.float32
MESH = pl.DeviceIdType.MESH
NT = (((1,), (1,)), ((), ()))


def _dot(a, b):
    return jnp.dot(a, b, preferred_element_type=F32)


def _dot_nt(a, b):
    return lax.dot_general(a, b, NT, preferred_element_type=F32)


def _kernel(n_total, kern_width, step_size,
            theta_in, prec_in, mean_in, fact_in, out_ref,
            th, tb, tsib, ab, gp, fr, cr, zr, kp, k2, zall, zrcv, sfull, sown, sbuf, prec_ref, mean_ref, u0_ref, u1_ref, par_s, sx_s, sx_r,
            in_s, in_r, tx_s, tx_r, zx_s, zx_r, fy_s, fy_r, ch_s, ch_r, zy_s, zy_r,
            kc_s, kc_r, ky_s, ky_r, kx_s, kx_r, out_s, out_r):
    z = lax.axis_index("part")
    f = lax.axis_index("feat")
    y = f // 2
    c = f % 2
    width = th.shape[1]
    half = n_total // 2
    group = n_total // 4

    def dev(zz, yy, cc):
        return {"part": zz, "feat": 2 * yy + cc}

    me = dev(z, y, c)
    ynb = dev(z, 1 - y, c)
    sib = dev(z, y, 1 - c)
    is_end = jnp.logical_or(z == 0, z == 3)
    is_mid = jnp.logical_not(is_end)
    e1 = jnp.where(z < 2, 1, 0)
    e2 = 1 - e1

    def toward(e):
        return dev(jnp.clip(z + 2 * e - 1, 0, 3), y, c)

    def away(e):
        return dev(jnp.clip(z - 2 * e + 1, 0, 3), y, c)

    def rc(src, dst, ss, rs, d):
        return pltpu.make_async_remote_copy(src_ref=src, dst_ref=dst, send_sem=ss, recv_sem=rs,
                                            device_id=d, device_id_type=MESH)

    bar = pltpu.get_barrier_semaphore()
    for k in range(1, 4):
        pl.semaphore_signal(bar, inc=1, device_id=dev((z + k) % 4, y, c), device_id_type=MESH)
    for k in range(4):
        pl.semaphore_signal(bar, inc=1, device_id=dev((z + k) % 4, 1 - y, c), device_id_type=MESH)
    pl.semaphore_signal(bar, inc=1, device_id=sib, device_id_type=MESH)
    pl.semaphore_wait(bar, 8)

    mine = pl.ds(pl.multiple_of(z * width, BLK), width)
    rank = fact_in.shape[0]
    pars = (pltpu.make_async_copy(prec_in.at[:, mine], prec_ref, par_s.at[0]),
            pltpu.make_async_copy(mean_in.at[:, mine], mean_ref, par_s.at[1]),
            pltpu.make_async_copy(fact_in.at[:, mine], u0_ref.at[pl.ds(0, rank), :], par_s.at[2]),
            pltpu.make_async_copy(fact_in.at[:, mine], u1_ref.at[pl.ds(HR, rank), :], par_s.at[3]))

    def grp(zz):
        return pl.multiple_of(((zz + 4 - 2 * c) % 4) * group, group)

    def in_copy(zz):
        return rc(theta_in.at[:, pl.ds(pl.multiple_of(zz * width, BLK), width)], th.at[pl.ds(grp(z), group), :],
                  in_s.at[zz], in_r.at[z], dev(zz, y, c))

    def in_local():
        return pltpu.make_async_copy(theta_in.at[:, pl.ds(pl.multiple_of(z * width, BLK), width)],
                                     th.at[pl.ds(grp(z), group), :], in_r.at[z])

    in_local().start()
    for dist in (3, 2, 1):
        for zz in (z + dist, z - dist):
            @pl.when(jnp.logical_and(zz >= 0, zz < 4))
            def _(zz=zz):
                in_copy(zz).start()

    for p in pars:
        p.start()
    u0_ref[HR:BLK, :] = jnp.zeros((HR, width), BF)
    u1_ref[0:HR, :] = jnp.zeros((HR, width), BF)
    if rank < HR:
        u0_ref[rank:HR, :] = jnp.zeros((HR - rank, width), BF)
        u1_ref[HR + rank:BLK, :] = jnp.zeros((HR - rank, width), BF)
    for p in pars:
        p.wait()

    def t_copy(par, i):
        src = tb.at[par, pl.ds(pl.multiple_of(i * TILE, TILE), TILE), :]
        dst = tsib.at[pl.ds(pl.multiple_of(((i + 4) % 8) * TILE, TILE), TILE), :]
        return rc(src, dst, tx_s.at[i], tx_r.at[(i + 4) % 8], sib)

    def z_copy():
        return rc(zall.at[pl.ds(8, 9)], zrcv, zx_s, zx_r, sib)

    eye = (lax.broadcasted_iota(jnp.int32, (BLK, BLK), 0) == lax.broadcasted_iota(jnp.int32, (BLK, BLK), 1))

    def finish_rows(i, par):
        rows = pl.ds(pl.multiple_of(i * TILE, TILE), TILE)
        tt = th[rows, :].astype(BF)
        tb[par, rows, :] = tt
        z_tile = _dot_nt((th[rows, :] - mean_ref[...]).astype(BF), u0_ref[...])
        low_lanes = lax.broadcasted_iota(jnp.int32, (HR, BLK), 1) < HR
        for s in range(TILE // BLK):
            b = i * (TILE // BLK) + s
            t_blk = tt[s * BLK:(s + 1) * BLK].astype(F32)
            s_col = jnp.sum(t_blk * t_blk, axis=1, keepdims=True)
            s_row = jnp.sum(jnp.where(eye, jnp.broadcast_to(s_col, (BLK, BLK)), 0.0), axis=0, keepdims=True)
            zall[16, pl.ds(b, 1), :] = s_row
            z_blk = z_tile[s * BLK:(s + 1) * BLK]
            zall[b] = jnp.where(low_lanes, z_blk[:HR], pltpu.roll(z_blk[HR:], HR, 1))

    def first_rows(k, carry):
        zz = (z + k) % 4

        @pl.when(k == 0)
        def _():
            in_local().wait()

        @pl.when(k > 0)
        def _():
            rc(th.at[pl.ds(grp(zz), group), :], th.at[pl.ds(grp(zz), group), :], in_s.at[zz], in_r.at[zz], me).wait_recv()
        for s in range(group // TILE):
            i = ((zz + 4 - 2 * c) % 4) * (group // TILE) + s
            finish_rows(i, 0)
            t_copy(0, i).start()
        return carry

    lax.fori_loop(0, 4, first_rows, 0)
    z_copy().start()
    for k in range(1, 4):
        in_copy((z + k) % 4).wait_send()

    def qf(yy, e):
        return yy * 2 + e

    def qz(yy, e):
        return 4 + yy * 2 + e

    def crow(i):
        return pl.ds(i * CH, CH)

    def fy_copy(e, i):
        return rc(gp.at[qf(1 - y, e), crow(i), :], fr.at[e, crow(i), :], fy_s.at[e, i], fy_r.at[e, i], ynb)

    def s_copy(yy, e, k):
        return rc(sown, sbuf.at[2 * z + y], sx_s.at[k], sx_r.at[2 * z + y], dev(3 * e, yy, c))

    def chain_q(n, e):
        return (qz(1 - y, e), qz(y, e), qf(y, e))[n // NCH]

    def chain_copy(n, e):
        return rc(gp.at[chain_q(n, e), crow(n % NCH), :], cr.at[e, n], ch_s.at[e, n], ch_r.at[e, n], toward(e))

    def zy_copy(i):
        return rc(gp.at[qz(1 - y, e2), crow(i), :], zr.at[crow(i), :], zy_s.at[i], zy_r.at[i], ynb)

    def krow(ch):
        return pl.ds(ch * (BLK // KCH), BLK // KCH)

    def kc_copy(e, j, ch, q):
        return rc(kp.at[0, q, krow(ch), :], kp.at[0, q, krow(ch), :], kc_s.at[e, j * KCH + ch], kc_r.at[e, j * KCH + ch], away(e))

    def ky_copy(e, kind, ch, q):
        return rc(kp.at[0, q, krow(ch), :], kp.at[0, q, krow(ch), :], ky_s.at[e, kind, ch], ky_r.at[e, kind, ch], ynb)

    def kx_copy(ch, q):
        return rc(kp.at[0, q, krow(ch), :], kp.at[1, q, krow(ch), :], kx_s.at[q, ch], kx_r.at[q, ch], sib)

    def step(t, carry):
        par = t % 2

        def own_part(q):
            rows = pl.ds(pl.multiple_of(q * BLK, BLK), BLK)
            win = pl.ds(pl.multiple_of(q * BLK, BLK), PW)
            return _dot_nt(tb[par, rows, :], tb[par, win, :])

        def t_wait(i, cc):
            t_copy(par, i).wait()
            return cc

        first_q = qz(1 - y, e1)
        gp[first_q] = own_part(first_q)
        lax.fori_loop(0, 8, t_wait, 0)
        z_copy().wait()
        sown[0:8, :] = zall[16, 0:8, :] + zrcv[8, 8:16, :]
        sown[8:16, :] = zall[16, 8:16, :] + zrcv[8, 0:8, :]
        for e in range(2):
            s_copy(1 - y, e, 2 + e).start()

            @pl.when(z != 3 * e)
            def _(e=e):
                s_copy(y, e, e).start()

        def panel(q, gram=None):
            rows = pl.ds(pl.multiple_of(q * BLK, BLK), BLK)
            win = pl.ds(pl.multiple_of(q * BLK, BLK), PW)
            gram = (own_part(q) if gram is None else gram) + _dot_nt(tsib[rows, :], tsib[win, :])
            gp[q, :, 0:GW] = gram[:, 0:GW]
            last = gram[:, GW:PW]
            right = jnp.logical_and(c == 1, lax.broadcasted_iota(jnp.int32, (HR, BLK), 1) < HR)
            gp[q, 0:HR, GW:PW] = jnp.where(right, pltpu.roll(last[HR:], HR, 1), last[:HR])
            gp[q, HR:BLK, GW:PW] = zall[q] + zrcv[q]

        panel(first_q, gp[first_q])

        @pl.when(is_end)
        def _():
            for i in range(NCH):
                chain_copy(i, e1).start()

        def mk_panels(m, cc):
            e = jnp.where(m == 0, e1, e2)
            panel(jnp.where(m < 2, qf(1 - y, e), qz(1 - y, e)))

            @pl.when(jnp.logical_or(m == 0, jnp.logical_and(m == 1, is_mid)))
            def _():
                for i in range(NCH):
                    fy_copy(e, i).start()
            return cc

        lax.fori_loop(0, 3, mk_panels, 0)

        def late_panels(m, cc):
            e = jnp.where(m % 2 == 0, e1, e2)
            panel(jnp.where(m < 2, qz(y, e), qf(y, e)))

            @pl.when(jnp.logical_and(is_end, m == 0))
            def _():
                for i in range(NCH):
                    chain_copy(NCH + i, e1).start()
            return cc

        KR = BLK // KCH

        def s_column(q, first):
            diag = lax.broadcasted_iota(jnp.int32, (KR, BLK), 0) + first == lax.broadcasted_iota(jnp.int32, (KR, BLK), 1)
            return jnp.sum(jnp.where(diag, jnp.broadcast_to(sfull[pl.ds(q, 1), :], (KR, BLK)), 0.0), axis=1, keepdims=True)

        def kern(s_col, s_row, gram):
            return jnp.exp(jnp.maximum(s_col + s_row - 2.0 * gram, 0.0) * (-1.0 / kern_width)).astype(BF)

        def kern_chunk(q, ch):
            rows = slice(ch * KR, (ch + 1) * KR)
            s_col = s_column(q, ch * KR)
            for k in range(SPAN):
                cols = slice(k * BLK, (k + 1) * BLK)
                kp[0, q, rows, cols] = kern(s_col, sfull[pl.ds(q + k, 1), :], gp[q, rows, cols])
            if ch < KCH // 2:
                right = jnp.logical_and(c == 1, lax.broadcasted_iota(jnp.int32, (KR, BLK), 1) < HR)
                s_row = jnp.broadcast_to(sfull[pl.ds(q + SPAN, 1), :], (KR, BLK))
                kp[0, q, rows, GW:PW] = kern(jnp.where(right, s_column(q, HR + ch * KR), s_col),
                                             jnp.where(right, pltpu.roll(s_row, HR, 1), s_row), gp[q, rows, GW:PW])
            else:
                kp[0, q, rows, GW:PW] = gp[q, rows, GW:PW].astype(BF)

        def send_own(j, q, ch):
            kern_chunk(q, ch)
            kc_copy(e2, j, ch, q).start()
            ky_copy(e2, 1 if j == 0 else 0, ch, q).start()
            kx_copy(ch, q).start()

        def take(n, e, with_chain, with_y):
            i = n % NCH
            rows = crow(i)
            q = chain_q(n, e)
            val = gp[q, rows, :]
            if with_y:
                rc(fr.at[e, rows, :], fr.at[e, rows, :], fy_s.at[e, i], fy_r.at[e, i], me).wait_recv()
                val = val + fr[e, rows, :]
            if with_chain:
                rc(cr.at[e, n], cr.at[e, n], ch_s.at[e, n], ch_r.at[e, n], me).wait_recv()
                val = val + cr[e, n]
            gp[q, rows, :] = val

        def panel_q(j, e):
            return jnp.where(j == 0, qz(y, e), jnp.where(j == 1, qf(y, e), qz(1 - y, e)))

        def k_take(m, e, fwd):
            j, ch = m // KCH, m % KCH
            q = panel_q(j, e)
            rows = pl.ds(pl.multiple_of(ch * (BLK // KCH), BLK // KCH), BLK // KCH)
            buf = kp.at[0, q, rows, :]
            rc(buf, buf, kc_s.at[e, m], kc_r.at[e, m], me).wait_recv()
            if fwd:
                rc(buf, buf, kc_s.at[e, m], kc_r.at[e, m], away(e)).start()

            @pl.when(j == 1)
            def _():
                rc(buf, buf, ky_s.at[e, 0, ch], ky_r.at[e, 0, ch], ynb).start()
            rc(buf, kp.at[1, q, rows, :], kx_s.at[q, ch], kx_r.at[q, ch], sib).start()

        def mid_round(m):
            for n, e in ((m, e1), (m - SKEW, e2)):
                if 0 <= n < 3 * NCH:
                    take(n, e, True, n >= 2 * NCH)
                    chain_copy(n, e).start()
                elif n >= 3 * NCH:
                    k_take(jnp.int32(n - 3 * NCH), e2, True)

        def end_round(n):
            if FSTART <= n < FSTART + NCH // 2:
                for k in range(2):
                    nn = 2 * NCH + 2 * (n - FSTART) + k
                    take(nn, e1, False, True)
                    chain_copy(nn, e1).start()
            take(n, e2, True, n >= 2 * NCH)
            if n < NCH:
                zy_copy(n).start()
            if NCH <= n < 2 * NCH:
                i = n - NCH
                rows = crow(i)
                rc(zr.at[rows, :], zr.at[rows, :], zy_s.at[i], zy_r.at[i], me).wait_recv()
                q = qz(y, e2)
                gp[q, rows, :] = gp[q, rows, :] + zr[rows, :]
                if n == NCH:
                    sfull[...] = sown[...]
                    for k in range(8):
                        @pl.when(2 * z + y != k)
                        def _(k=k):
                            rc(sbuf.at[k], sbuf.at[k], sx_s.at[0], sx_r.at[k], me).wait_recv()
                            sfull[...] = sfull[...] + sbuf[k]
            if NCH - 1 <= n < 2 * NCH - 1:
                fy_copy(e2, n - NCH + 1).start()
            per = NCH // KCH
            if n >= NCH and n % per == per - 1:
                if n < 2 * NCH:
                    send_own(0, qz(y, e2), (n - NCH) // per)
                else:
                    send_own(1, qf(y, e2), (n - 2 * NCH) // per)
            if n in YFWD:
                ch = YFWD.index(n)
                q = qz(1 - y, e2)
                buf = kp.at[0, q, krow(ch), :]
                rc(buf, buf, ky_s.at[e2, 1, ch], ky_r.at[e2, 1, ch], me).wait_recv()
                kc_copy(e2, 2, ch, q).start()
                kx_copy(ch, q).start()

        @pl.when(is_mid)
        def _():
            for m in range(3 * NCH + SKEW):
                if m < 4:
                    lax.fori_loop(m, m + 1, late_panels, 0)
                mid_round(m)

        @pl.when(is_end)
        def _():
            lax.fori_loop(0, 4, late_panels, 0)
            for n in range(3 * NCH):
                end_round(n)

        def assemble(h, q):
            lo = pl.ds(pl.multiple_of(q * BLK, BLK), BLK)
            for k in range(SPAN):
                blk = kp[h, q, :, k * BLK:(k + 1) * BLK]
                k2[h, lo, pl.ds(pl.multiple_of((q + k) * BLK, BLK), BLK)] = blk
                if k >= 1:
                    flip = (q + k) // 8
                    k2[(h + flip) % 2, pl.ds(pl.multiple_of((q + k - 8 * flip) * BLK, BLK), BLK),
                       pl.ds(pl.multiple_of((q + 8 * flip) * BLK, BLK), BLK)] = blk.T
            zb = kp[h, q, HR:BLK, GW:PW]
            for s, u_ref in ((0, u0_ref), (1, u1_ref)):
                rows = pl.ds(pl.multiple_of((h * 8 + q) * BLK + s * HR, HR), HR)
                low = _dot(zb, u_ref[...])
                x_dev = th[rows, :] - mean_ref[...]
                ab[rows, :] = (-(x_dev * prec_ref[...] + low)).astype(BF)

        def pair_block(q):
            upper = kp[c, q, 0:HR, GW:PW].astype(F32)
            right = kp[1 - c, q, 0:HR, GW:PW].astype(F32)
            lower = jnp.concatenate([right, pltpu.roll(right, HR, 1)], axis=0).T[HR:BLK]
            blk = jnp.concatenate([upper, lower], axis=0)
            rows = pl.ds(pl.multiple_of(q * BLK, BLK), BLK)
            cols = pl.ds(pl.multiple_of((q + SPAN) * BLK, BLK), BLK)
            k2[c, rows, cols] = blk.astype(BF)
            k2[1 - c, rows, cols] = blk.T.astype(BF)

        def from_sib(q):
            for ch in range(KCH):
                buf = kp.at[1, q, krow(ch), :]
                rc(buf, buf, kx_s.at[q, ch], kx_r.at[q, ch], me).wait_recv()
            assemble(1, q)
            pair_block(q)

        def from_y(e):
            q = qf(1 - y, e)
            for ch in range(KCH):
                buf = kp.at[0, q, krow(ch), :]
                rc(buf, buf, ky_s.at[e, 0, ch], ky_r.at[e, 0, ch], me).wait_recv()
                kx_copy(ch, q).start()
            assemble(0, q)

        def k_round(m, cc):
            near = m + SKEW < 3 * KCH
            nn = jnp.minimum(m + SKEW, 3 * KCH - 1)

            @pl.when(jnp.logical_and(near, is_mid))
            def _():
                k_take(nn, e2, True)

            @pl.when(is_mid)
            def _():
                k_take(m, e1, True)

            @pl.when(is_end)
            def _():
                k_take(m, e1, False)

            @pl.when(jnp.logical_and(near, nn % KCH == KCH - 1))
            def _():
                assemble(0, panel_q(nn // KCH, e2))

            @pl.when(jnp.logical_and(near, jnp.logical_and(nn % KCH == KCH - 1, nn >= KCH)))
            def _():
                from_sib(panel_q(nn // KCH - 1, e2))

            @pl.when(m % KCH == KCH - 1)
            def _():
                assemble(0, panel_q(m // KCH, e1))

            @pl.when(jnp.logical_and(m % KCH == KCH - 1, m >= KCH))
            def _():
                from_sib(panel_q(m // KCH - 1, e1))

            @pl.when(m == 2 * KCH)
            def _():
                from_y(e2)

            @pl.when(m == 2 * KCH + 1)
            def _():
                from_y(e1)

            @pl.when(m == 2 * KCH + 2)
            def _():
                from_sib(qf(1 - y, e2))
            return cc

        lax.fori_loop(0, 3 * KCH, k_round, 0)

        def last_sib(k, cc):
            from_sib(jnp.where(k == 0, qf(1 - y, e1), jnp.where(k == 1, panel_q(2, e2), panel_q(2, e1))))
            return cc

        lax.fori_loop(0, 3, last_sib, 0)

        for e in range(2):
            s_copy(1 - y, e, 2 + e).wait_send()

            @pl.when(z != 3 * e)
            def _(e=e):
                s_copy(y, e, e).wait_send()
            for i in range(NCH):
                fy_copy(e, i).wait_send()
        for n in range(3 * NCH):
            chain_copy(n, e1).wait_send()

            @pl.when(is_mid)
            def _(n=n):
                chain_copy(n, e2).wait_send()

        @pl.when(is_end)
        def _():
            for i in range(NCH):
                zy_copy(i).wait_send()

        def tile_of(k):
            low = z < 2
            zm = jnp.where(low, z, 3 - z)
            zo = jnp.where(k < 2, 2, jnp.where(k < 4, 3, jnp.where(k < 6, 1 - zm, zm)))
            zz = jnp.where(low, zo, 3 - zo)
            return zz, ((zz + 4 - 2 * c) % 4) * 2 + k % 2

        def phi_tile(k, cc):
            zz, i = tile_of(k)
            _, done = tile_of(jnp.maximum(k - 1, 0))
            finish_rows(done, 1 - par)
            h = i // 4
            rows = pl.ds(pl.multiple_of(i * TILE, TILE), TILE)
            krows = pl.ds(pl.multiple_of((i % 4) * TILE, TILE), TILE)
            first = pl.ds(pl.multiple_of(h * half, half), half)
            second = pl.ds(pl.multiple_of((1 - h) * half, half), half)
            ka = k2[h, krows, 0:half]
            kb = k2[h, krows, half:n_total]
            drive = _dot(ka, ab[first, :]) + _dot(kb, ab[second, :])
            pull = _dot(ka, tb[par, first, :]) + _dot(kb, tb[par, second, :])
            mass = jnp.sum(ka.astype(F32), axis=1, keepdims=True) + jnp.sum(kb.astype(F32), axis=1, keepdims=True)
            t_own = tb[par, rows, :].astype(F32)
            upd = (drive + (2.0 / kern_width) * (mass * t_own - pull)) * (1.0 / n_total)
            th[rows, :] = th[rows, :] + step_size * upd

            @pl.when(jnp.logical_and(t < NUM_STEPS - 1, k > 0))
            def _():
                t_copy(1 - par, done).start()

            @pl.when(t == NUM_STEPS - 1)
            def _():
                dst = out_ref.at[pl.ds(pl.multiple_of((i % 2) * TILE, TILE), TILE), pl.ds(pl.multiple_of(z * width, BLK), width)]

                @pl.when(zz == z)
                def _():
                    pltpu.make_async_copy(th.at[rows, :], dst, out_s.at[i]).start()

                @pl.when(zz != z)
                def _():
                    rc(th.at[rows, :], dst, out_s.at[i], out_r.at[z, i % 2], dev(zz, y, c)).start()
            return cc

        lax.fori_loop(0, 8, phi_tile, 0)

        @pl.when(t < NUM_STEPS - 1)
        def _():
            _, done = tile_of(7)
            finish_rows(done, 1 - par)
            t_copy(1 - par, done).start()
            z_copy().start()

        for ch in range(KCH):
            for e in range(2):
                ky_copy(e, 0, ch, qf(y, e)).wait_send()

            @pl.when(is_end)
            def _(ch=ch):
                ky_copy(e2, 1, ch, qz(y, e2)).wait_send()
            for j in range(3):
                q2 = (qz(y, e2), qf(y, e2), qz(1 - y, e2))[j]
                q1 = (qz(y, e1), qf(y, e1), qz(1 - y, e1))[j]
                kc_copy(e2, j, ch, q2).wait_send()

                @pl.when(is_mid)
                def _(ch=ch, j=j, q1=q1):
                    kc_copy(e1, j, ch, q1).wait_send()
            for q in range(8):
                kx_copy(ch, q).wait_send()
        return carry

    lax.fori_loop(0, NUM_STEPS, step, 0)

    def out_wait(i, cc):
        zz = (i // 2 + 2 * c) % 4
        rows = pl.ds(pl.multiple_of(i * TILE, TILE), TILE)
        dst = out_ref.at[pl.ds(pl.multiple_of((i % 2) * TILE, TILE), TILE), pl.ds(pl.multiple_of(z * width, BLK), width)]

        @pl.when(zz == z)
        def _():
            pltpu.make_async_copy(th.at[rows, :], dst, out_s.at[i]).wait()

        @pl.when(zz != z)
        def _():
            rc(th.at[rows, :], dst, out_s.at[i], out_r.at[z, i % 2], dev(zz, y, c)).wait_send()
        return cc

    lax.fori_loop(0, 8, out_wait, 0)
    for k in range(1, 4):
        zz = (z + k) % 4
        for s in range(2):
            dst = out_ref.at[pl.ds(s * TILE, TILE), pl.ds(pl.multiple_of(zz * width, BLK), width)]
            rc(dst, dst, out_s.at[0], out_r.at[zz, s], me).wait_recv()


def solution(mesh):
    part_size = mesh.shape["part"]
    feat_size = mesh.shape["feat"]

    def local_steps(local_theta, prec_loc, mean_loc, factor_loc):
        rows_loc, feat_loc = local_theta.shape
        n_total = rows_loc * part_size
        feat_total = feat_loc * feat_size
        width = feat_loc // part_size
        kern_width = 2.0 * feat_total / math.log(n_total)
        step_size = 0.15 * n_total * feat_total / math.log(n_total)
        anym = pl.BlockSpec(memory_space=pl.ANY)
        dma = pltpu.SemaphoreType.DMA
        body = lambda *refs: _kernel(n_total, kern_width, step_size, *refs)
        return pl.pallas_call(
            body,
            out_shape=pltpu.VMEM((rows_loc, feat_loc), F32),
            in_specs=[anym, anym, anym, anym],
            out_specs=pl.BlockSpec(memory_space=pltpu.VMEM),
            scratch_shapes=[
                pltpu.VMEM((n_total, width), F32),
                pltpu.VMEM((2, n_total, width), BF),
                pltpu.VMEM((n_total, width), BF),
                pltpu.VMEM((n_total, width), BF),
                pltpu.VMEM((8, BLK, PW), F32),
                pltpu.VMEM((2, BLK, PW), F32),
                pltpu.VMEM((2, 3 * NCH, CH, PW), F32),
                pltpu.VMEM((BLK, PW), F32),
                pltpu.VMEM((2, 8, BLK, PW), BF),
                pltpu.VMEM((2, n_total // 2, n_total), BF),
                pltpu.VMEM((17, HR, BLK), F32),
                pltpu.VMEM((9, HR, BLK), F32),
                pltpu.VMEM((16, BLK), F32), pltpu.VMEM((16, BLK), F32), pltpu.VMEM((8, 16, BLK), F32),
                pltpu.VMEM((1, width), F32), pltpu.VMEM((1, width), F32),
                pltpu.VMEM((BLK, width), BF), pltpu.VMEM((BLK, width), BF),
                dma((4,)), dma((4,)), dma((8,)),
                dma((4,)), dma((4,)), dma((8,)), dma((8,)), dma, dma,
                dma((2, NCH)), dma((2, NCH)), dma((2, 3 * NCH)), dma((2, 3 * NCH)), dma((NCH,)), dma((NCH,)),
                dma((2, 3 * KCH)), dma((2, 3 * KCH)), dma((2, 2, KCH)), dma((2, 2, KCH)), dma((8, KCH)), dma((8, KCH)),
                dma((8,)), dma((4, 2)),
            ],
            compiler_params=pltpu.CompilerParams(collective_id=0, has_side_effects=True, vmem_limit_bytes=54 * 1024 * 1024),
            name="svgd",
        )(local_theta, prec_loc[None, :], mean_loc[None, :], factor_loc.T)

    row_spec = P(("ens", "part"), "feat")
    vec_spec = P(("ens", "feat"))
    fac_spec = P(("ens", "feat"), None)
    return jax.shard_map(local_steps, mesh=mesh, in_specs=(row_spec, vec_spec, vec_spec, fac_spec), out_specs=row_spec, check_vma=False)
```

```python
import math
import jax
import jax.numpy as jnp
from jax import lax
from jax.experimental import pallas as pl
from jax.experimental.pallas import tpu as pltpu
from jax.sharding import PartitionSpec as P

NUM_STEPS = 3
BLK = 128
SPAN = 8
PW = (SPAN + 1) * BLK
GW = SPAN * BLK
NCH = 8
CH = BLK // NCH
KCH = 4
HR = BLK // 2
FSTART = 4
YFWD = (17, 20, 22, 23)
SKEW = 2
TILE = 256
BF = jnp.bfloat16
F32 = jnp.float32
MESH = pl.DeviceIdType.MESH
NT = (((1,), (1,)), ((), ()))


def _dot(a, b):
    return jnp.dot(a, b, preferred_element_type=F32)


def _dot_nt(a, b):
    return lax.dot_general(a, b, NT, preferred_element_type=F32)


def _kernel(n_total, kern_width, step_size,
            theta_in, prec_in, mean_in, fact_in, out_ref,
            th, tb, tsib, ab, gp, fr, cr, zr, kp, k2, zall, zrcv, sfull, sown, sbuf, prec_ref, mean_ref, u0_ref, u1_ref, par_s, sx_s, sx_r,
            in_s, in_r, tx_s, tx_r, zx_s, zx_r, fy_s, fy_r, ch_s, ch_r, zy_s, zy_r,
            kc_s, kc_r, ky_s, ky_r, kx_s, kx_r, out_s, out_r):
    z = lax.axis_index("part")
    f = lax.axis_index("feat")
    y = f // 2
    c = f % 2
    width = th.shape[1]
    half = n_total // 2
    group = n_total // 4

    def dev(zz, yy, cc):
        return {"part": zz, "feat": 2 * yy + cc}

    me = dev(z, y, c)
    ynb = dev(z, 1 - y, c)
    sib = dev(z, y, 1 - c)
    is_end = jnp.logical_or(z == 0, z == 3)
    is_mid = jnp.logical_not(is_end)
    e1 = jnp.where(z < 2, 1, 0)
    e2 = 1 - e1

    def toward(e):
        return dev(jnp.clip(z + 2 * e - 1, 0, 3), y, c)

    def away(e):
        return dev(jnp.clip(z - 2 * e + 1, 0, 3), y, c)

    def rc(src, dst, ss, rs, d):
        return pltpu.make_async_remote_copy(src_ref=src, dst_ref=dst, send_sem=ss, recv_sem=rs,
                                            device_id=d, device_id_type=MESH)

    bar = pltpu.get_barrier_semaphore()
    for k in range(1, 4):
        pl.semaphore_signal(bar, inc=1, device_id=dev((z + k) % 4, y, c), device_id_type=MESH)
    for k in range(4):
        pl.semaphore_signal(bar, inc=1, device_id=dev((z + k) % 4, 1 - y, c), device_id_type=MESH)
    pl.semaphore_signal(bar, inc=1, device_id=sib, device_id_type=MESH)
    pl.semaphore_wait(bar, 8)

    mine = pl.ds(pl.multiple_of(z * width, BLK), width)
    rank = fact_in.shape[0]
    pars = (pltpu.make_async_copy(prec_in.at[:, mine], prec_ref, par_s.at[0]),
            pltpu.make_async_copy(mean_in.at[:, mine], mean_ref, par_s.at[1]),
            pltpu.make_async_copy(fact_in.at[:, mine], u0_ref.at[pl.ds(0, rank), :], par_s.at[2]),
            pltpu.make_async_copy(fact_in.at[:, mine], u1_ref.at[pl.ds(HR, rank), :], par_s.at[3]))

    def grp(zz):
        return pl.multiple_of(((zz + 4 - 2 * c) % 4) * group, group)

    def in_copy(zz):
        return rc(theta_in.at[:, pl.ds(pl.multiple_of(zz * width, BLK), width)], th.at[pl.ds(grp(z), group), :],
                  in_s.at[zz], in_r.at[z], dev(zz, y, c))

    def in_local():
        return pltpu.make_async_copy(theta_in.at[:, pl.ds(pl.multiple_of(z * width, BLK), width)],
                                     th.at[pl.ds(grp(z), group), :], in_r.at[z])

    in_local().start()
    for dist in (3, 2, 1):
        for zz in (z + dist, z - dist):
            @pl.when(jnp.logical_and(zz >= 0, zz < 4))
            def _(zz=zz):
                in_copy(zz).start()

    for p in pars:
        p.start()
    u0_ref[HR:BLK, :] = jnp.zeros((HR, width), BF)
    u1_ref[0:HR, :] = jnp.zeros((HR, width), BF)
    if rank < HR:
        u0_ref[rank:HR, :] = jnp.zeros((HR - rank, width), BF)
        u1_ref[HR + rank:BLK, :] = jnp.zeros((HR - rank, width), BF)
    for p in pars:
        p.wait()

    def t_copy(par, i):
        src = tb.at[par, pl.ds(pl.multiple_of(i * TILE, TILE), TILE), :]
        dst = tsib.at[pl.ds(pl.multiple_of(((i + 4) % 8) * TILE, TILE), TILE), :]
        return rc(src, dst, tx_s.at[i], tx_r.at[(i + 4) % 8], sib)

    def z_copy():
        return rc(zall.at[pl.ds(8, 9)], zrcv, zx_s, zx_r, sib)

    eye = (lax.broadcasted_iota(jnp.int32, (BLK, BLK), 0) == lax.broadcasted_iota(jnp.int32, (BLK, BLK), 1))

    def finish_rows(i, par):
        rows = pl.ds(pl.multiple_of(i * TILE, TILE), TILE)
        tt = th[rows, :].astype(BF)
        tb[par, rows, :] = tt
        z_tile = _dot_nt((th[rows, :] - mean_ref[...]).astype(BF), u0_ref[...])
        low_lanes = lax.broadcasted_iota(jnp.int32, (HR, BLK), 1) < HR
        for s in range(TILE // BLK):
            b = i * (TILE // BLK) + s
            t_blk = tt[s * BLK:(s + 1) * BLK].astype(F32)
            s_col = jnp.sum(t_blk * t_blk, axis=1, keepdims=True)
            s_row = jnp.sum(jnp.where(eye, jnp.broadcast_to(s_col, (BLK, BLK)), 0.0), axis=0, keepdims=True)
            zall[16, pl.ds(b, 1), :] = s_row
            z_blk = z_tile[s * BLK:(s + 1) * BLK]
            zall[b] = jnp.where(low_lanes, z_blk[:HR], pltpu.roll(z_blk[HR:], HR, 1))

    def first_rows(k, carry):
        partner = jnp.where(z < 2, 1 - z, 5 - z)
        zz = jnp.where(k == 0, z, jnp.where(k == 1, partner, jnp.where(k == 2, (z + 2) % 4, (partner + 2) % 4)))

        @pl.when(k == 0)
        def _():
            in_local().wait()

        @pl.when(k > 0)
        def _():
            rc(th.at[pl.ds(grp(zz), group), :], th.at[pl.ds(grp(zz), group), :], in_s.at[zz], in_r.at[zz], me).wait_recv()
        for s in range(group // TILE):
            i = ((zz + 4 - 2 * c) % 4) * (group // TILE) + s
            finish_rows(i, 0)
            t_copy(0, i).start()
        return carry

    lax.fori_loop(0, 4, first_rows, 0)
    z_copy().start()
    def qf(yy, e):
        return yy * 2 + e

    def qz(yy, e):
        return 4 + yy * 2 + e

    def crow(i):
        return pl.ds(i * CH, CH)

    def fy_copy(e, i):
        return rc(gp.at[qf(1 - y, e), crow(i), :], fr.at[e, crow(i), :], fy_s.at[e, i], fy_r.at[e, i], ynb)

    def s_copy(yy, e, k):
        return rc(sown, sbuf.at[2 * z + y], sx_s.at[k], sx_r.at[2 * z + y], dev(3 * e, yy, c))

    def chain_q(n, e):
        return (qz(1 - y, e), qz(y, e), qf(y, e))[n // NCH]

    def chain_copy(n, e):
        return rc(gp.at[chain_q(n, e), crow(n % NCH), :], cr.at[e, n], ch_s.at[e, n], ch_r.at[e, n], toward(e))

    def zy_copy(i):
        return rc(gp.at[qz(1 - y, e2), crow(i), :], zr.at[crow(i), :], zy_s.at[i], zy_r.at[i], ynb)

    def krow(ch):
        return pl.ds(ch * (BLK // KCH), BLK // KCH)

    def kc_copy(e, j, ch, q):
        return rc(kp.at[0, q, krow(ch), :], kp.at[0, q, krow(ch), :], kc_s.at[e, j * KCH + ch], kc_r.at[e, j * KCH + ch], away(e))

    def ky_copy(e, kind, ch, q):
        return rc(kp.at[0, q, krow(ch), :], kp.at[0, q, krow(ch), :], ky_s.at[e, kind, ch], ky_r.at[e, kind, ch], ynb)

    def kx_copy(ch, q):
        return rc(kp.at[0, q, krow(ch), :], kp.at[1, q, krow(ch), :], kx_s.at[q, ch], kx_r.at[q, ch], sib)

    def step(t, carry):
        par = t % 2

        def own_part(q):
            rows = pl.ds(pl.multiple_of(q * BLK, BLK), BLK)
            win = pl.ds(pl.multiple_of(q * BLK, BLK), PW)
            return _dot_nt(tb[par, rows, :], tb[par, win, :])

        def t_wait(i, cc):
            t_copy(par, i).wait()
            return cc

        first_q = qz(1 - y, e1)
        gp[first_q] = own_part(first_q)
        lax.fori_loop(0, 8, t_wait, 0)
        z_copy().wait()
        sown[0:8, :] = zall[16, 0:8, :] + zrcv[8, 8:16, :]
        sown[8:16, :] = zall[16, 8:16, :] + zrcv[8, 0:8, :]
        for e in range(2):
            s_copy(1 - y, e, 2 + e).start()

            @pl.when(z != 3 * e)
            def _(e=e):
                s_copy(y, e, e).start()

        def panel(q, gram=None):
            rows = pl.ds(pl.multiple_of(q * BLK, BLK), BLK)
            win = pl.ds(pl.multiple_of(q * BLK, BLK), PW)
            gram = (own_part(q) if gram is None else gram) + _dot_nt(tsib[rows, :], tsib[win, :])
            gp[q, :, 0:GW] = gram[:, 0:GW]
            last = gram[:, GW:PW]
            right = jnp.logical_and(c == 1, lax.broadcasted_iota(jnp.int32, (HR, BLK), 1) < HR)
            gp[q, 0:HR, GW:PW] = jnp.where(right, pltpu.roll(last[HR:], HR, 1), last[:HR])
            gp[q, HR:BLK, GW:PW] = zall[q] + zrcv[q]

        panel(first_q, gp[first_q])

        @pl.when(is_end)
        def _():
            for i in range(NCH):
                chain_copy(i, e1).start()

        def mk_panels(m, cc):
            e = jnp.where(m == 0, e1, e2)
            panel(jnp.where(m < 2, qf(1 - y, e), qz(1 - y, e)))

            @pl.when(jnp.logical_or(m == 0, jnp.logical_and(m == 1, is_mid)))
            def _():
                for i in range(NCH):
                    fy_copy(e, i).start()
            return cc

        lax.fori_loop(0, 3, mk_panels, 0)

        def late_panels(m, cc):
            e = jnp.where(m % 2 == 0, e1, e2)
            panel(jnp.where(m < 2, qz(y, e), qf(y, e)))

            @pl.when(jnp.logical_and(is_end, m == 0))
            def _():
                for i in range(NCH):
                    chain_copy(NCH + i, e1).start()
            return cc

        KR = BLK // KCH

        def s_column(q, first):
            diag = lax.broadcasted_iota(jnp.int32, (KR, BLK), 0) + first == lax.broadcasted_iota(jnp.int32, (KR, BLK), 1)
            return jnp.sum(jnp.where(diag, jnp.broadcast_to(sfull[pl.ds(q, 1), :], (KR, BLK)), 0.0), axis=1, keepdims=True)

        def kern(s_col, s_row, gram):
            return jnp.exp(jnp.maximum(s_col + s_row - 2.0 * gram, 0.0) * (-1.0 / kern_width)).astype(BF)

        def kern_chunk(q, ch):
            rows = slice(ch * KR, (ch + 1) * KR)
            s_col = s_column(q, ch * KR)
            for k in range(SPAN):
                cols = slice(k * BLK, (k + 1) * BLK)
                kp[0, q, rows, cols] = kern(s_col, sfull[pl.ds(q + k, 1), :], gp[q, rows, cols])
            if ch < KCH // 2:
                right = jnp.logical_and(c == 1, lax.broadcasted_iota(jnp.int32, (KR, BLK), 1) < HR)
                s_row = jnp.broadcast_to(sfull[pl.ds(q + SPAN, 1), :], (KR, BLK))
                kp[0, q, rows, GW:PW] = kern(jnp.where(right, s_column(q, HR + ch * KR), s_col),
                                             jnp.where(right, pltpu.roll(s_row, HR, 1), s_row), gp[q, rows, GW:PW])
            else:
                kp[0, q, rows, GW:PW] = gp[q, rows, GW:PW].astype(BF)

        def send_own(j, q, ch):
            kern_chunk(q, ch)
            kc_copy(e2, j, ch, q).start()
            ky_copy(e2, 1 if j == 0 else 0, ch, q).start()
            kx_copy(ch, q).start()

        def take(n, e, with_chain, with_y):
            i = n % NCH
            rows = crow(i)
            q = chain_q(n, e)
            val = gp[q, rows, :]
            if with_y:
                rc(fr.at[e, rows, :], fr.at[e, rows, :], fy_s.at[e, i], fy_r.at[e, i], me).wait_recv()
                val = val + fr[e, rows, :]
            if with_chain:
                rc(cr.at[e, n], cr.at[e, n], ch_s.at[e, n], ch_r.at[e, n], me).wait_recv()
                val = val + cr[e, n]
            gp[q, rows, :] = val

        def panel_q(j, e):
            return jnp.where(j == 0, qz(y, e), jnp.where(j == 1, qf(y, e), qz(1 - y, e)))

        def k_take(m, e, fwd):
            j, ch = m // KCH, m % KCH
            q = panel_q(j, e)
            rows = pl.ds(pl.multiple_of(ch * (BLK // KCH), BLK // KCH), BLK // KCH)
            buf = kp.at[0, q, rows, :]
            rc(buf, buf, kc_s.at[e, m], kc_r.at[e, m], me).wait_recv()
            if fwd:
                rc(buf, buf, kc_s.at[e, m], kc_r.at[e, m], away(e)).start()

            @pl.when(j == 1)
            def _():
                rc(buf, buf, ky_s.at[e, 0, ch], ky_r.at[e, 0, ch], ynb).start()
            rc(buf, kp.at[1, q, rows, :], kx_s.at[q, ch], kx_r.at[q, ch], sib).start()

        def mid_round(m):
            for n, e in ((m, e1), (m - SKEW, e2)):
                if 0 <= n < 3 * NCH:
                    take(n, e, True, n >= 2 * NCH)
                    chain_copy(n, e).start()
                elif n >= 3 * NCH:
                    k_take(jnp.int32(n - 3 * NCH), e2, True)

        def end_round(n):
            if FSTART <= n < FSTART + NCH // 2:
                for k in range(2):
                    nn = 2 * NCH + 2 * (n - FSTART) + k
                    take(nn, e1, False, True)
                    chain_copy(nn, e1).start()
            take(n, e2, True, n >= 2 * NCH)
            if n < NCH:
                zy_copy(n).start()
            if NCH <= n < 2 * NCH:
                i = n - NCH
                rows = crow(i)
                rc(zr.at[rows, :], zr.at[rows, :], zy_s.at[i], zy_r.at[i], me).wait_recv()
                q = qz(y, e2)
                gp[q, rows, :] = gp[q, rows, :] + zr[rows, :]
                if n == NCH:
                    sfull[...] = sown[...]
                    for k in range(8):
                        @pl.when(2 * z + y != k)
                        def _(k=k):
                            rc(sbuf.at[k], sbuf.at[k], sx_s.at[0], sx_r.at[k], me).wait_recv()
                            sfull[...] = sfull[...] + sbuf[k]
            if NCH - 1 <= n < 2 * NCH - 1:
                fy_copy(e2, n - NCH + 1).start()
            per = NCH // KCH
            if n >= NCH and n % per == per - 1:
                if n < 2 * NCH:
                    send_own(0, qz(y, e2), (n - NCH) // per)
                else:
                    send_own(1, qf(y, e2), (n - 2 * NCH) // per)
            if n in YFWD:
                ch = YFWD.index(n)
                q = qz(1 - y, e2)
                buf = kp.at[0, q, krow(ch), :]
                rc(buf, buf, ky_s.at[e2, 1, ch], ky_r.at[e2, 1, ch], me).wait_recv()
                kc_copy(e2, 2, ch, q).start()
                kx_copy(ch, q).start()

        @pl.when(is_mid)
        def _():
            for m in range(3 * NCH + SKEW):
                if m < 4:
                    lax.fori_loop(m, m + 1, late_panels, 0)
                mid_round(m)

        @pl.when(is_end)
        def _():
            lax.fori_loop(0, 4, late_panels, 0)
            for n in range(3 * NCH):
                end_round(n)

        def assemble(h, q):
            lo = pl.ds(pl.multiple_of(q * BLK, BLK), BLK)
            for k in range(SPAN):
                blk = kp[h, q, :, k * BLK:(k + 1) * BLK]
                k2[h, lo, pl.ds(pl.multiple_of((q + k) * BLK, BLK), BLK)] = blk
                if k >= 1:
                    flip = (q + k) // 8
                    k2[(h + flip) % 2, pl.ds(pl.multiple_of((q + k - 8 * flip) * BLK, BLK), BLK),
                       pl.ds(pl.multiple_of((q + 8 * flip) * BLK, BLK), BLK)] = blk.T
            zb = kp[h, q, HR:BLK, GW:PW]
            for s, u_ref in ((0, u0_ref), (1, u1_ref)):
                rows = pl.ds(pl.multiple_of((h * 8 + q) * BLK + s * HR, HR), HR)
                low = _dot(zb, u_ref[...])
                x_dev = th[rows, :] - mean_ref[...]
                ab[rows, :] = (-(x_dev * prec_ref[...] + low)).astype(BF)

        def pair_block(q):
            upper = kp[c, q, 0:HR, GW:PW].astype(F32)
            right = kp[1 - c, q, 0:HR, GW:PW].astype(F32)
            lower = jnp.concatenate([right, pltpu.roll(right, HR, 1)], axis=0).T[HR:BLK]
            blk = jnp.concatenate([upper, lower], axis=0)
            rows = pl.ds(pl.multiple_of(q * BLK, BLK), BLK)
            cols = pl.ds(pl.multiple_of((q + SPAN) * BLK, BLK), BLK)
            k2[c, rows, cols] = blk.astype(BF)
            k2[1 - c, rows, cols] = blk.T.astype(BF)

        def from_sib(q):
            for ch in range(KCH):
                buf = kp.at[1, q, krow(ch), :]
                rc(buf, buf, kx_s.at[q, ch], kx_r.at[q, ch], me).wait_recv()
            assemble(1, q)
            pair_block(q)

        def from_y(e):
            q = qf(1 - y, e)
            for ch in range(KCH):
                buf = kp.at[0, q, krow(ch), :]
                rc(buf, buf, ky_s.at[e, 0, ch], ky_r.at[e, 0, ch], me).wait_recv()
                kx_copy(ch, q).start()
            assemble(0, q)

        def k_round(m, cc):
            near = m + SKEW < 3 * KCH
            nn = jnp.minimum(m + SKEW, 3 * KCH - 1)

            @pl.when(jnp.logical_and(near, is_mid))
            def _():
                k_take(nn, e2, True)

            @pl.when(is_mid)
            def _():
                k_take(m, e1, True)

            @pl.when(is_end)
            def _():
                k_take(m, e1, False)

            @pl.when(jnp.logical_and(near, nn % KCH == KCH - 1))
            def _():
                assemble(0, panel_q(nn // KCH, e2))

            @pl.when(jnp.logical_and(near, jnp.logical_and(nn % KCH == KCH - 1, nn >= KCH)))
            def _():
                from_sib(panel_q(nn // KCH - 1, e2))

            @pl.when(m % KCH == KCH - 1)
            def _():
                assemble(0, panel_q(m // KCH, e1))

            @pl.when(jnp.logical_and(m % KCH == KCH - 1, m >= KCH))
            def _():
                from_sib(panel_q(m // KCH - 1, e1))

            @pl.when(m == 2 * KCH)
            def _():
                from_y(e2)

            @pl.when(m == 2 * KCH + 1)
            def _():
                from_y(e1)

            @pl.when(m == 2 * KCH + 2)
            def _():
                from_sib(qf(1 - y, e2))
            return cc

        lax.fori_loop(0, 3 * KCH, k_round, 0)

        def last_sib(k, cc):
            from_sib(jnp.where(k == 0, qf(1 - y, e1), jnp.where(k == 1, panel_q(2, e2), panel_q(2, e1))))
            return cc

        lax.fori_loop(0, 3, last_sib, 0)

        for e in range(2):
            s_copy(1 - y, e, 2 + e).wait_send()

            @pl.when(z != 3 * e)
            def _(e=e):
                s_copy(y, e, e).wait_send()
            for i in range(NCH):
                fy_copy(e, i).wait_send()
        for n in range(3 * NCH):
            chain_copy(n, e1).wait_send()

            @pl.when(is_mid)
            def _(n=n):
                chain_copy(n, e2).wait_send()

        @pl.when(is_end)
        def _():
            for i in range(NCH):
                zy_copy(i).wait_send()

        def tile_of(k):
            low = z < 2
            zm = jnp.where(low, z, 3 - z)
            zo = jnp.where(k < 2, 2, jnp.where(k < 4, 3, jnp.where(k < 6, 1 - zm, zm)))
            zz = jnp.where(low, zo, 3 - zo)
            return zz, ((zz + 4 - 2 * c) % 4) * 2 + k % 2

        def phi_tile(k, cc):
            zz, i = tile_of(k)
            _, done = tile_of(jnp.maximum(k - 1, 0))
            finish_rows(done, 1 - par)
            h = i // 4
            rows = pl.ds(pl.multiple_of(i * TILE, TILE), TILE)
            krows = pl.ds(pl.multiple_of((i % 4) * TILE, TILE), TILE)
            first = pl.ds(pl.multiple_of(h * half, half), half)
            second = pl.ds(pl.multiple_of((1 - h) * half, half), half)
            ka = k2[h, krows, 0:half]
            kb = k2[h, krows, half:n_total]
            drive = _dot(ka, ab[first, :]) + _dot(kb, ab[second, :])
            pull = _dot(ka, tb[par, first, :]) + _dot(kb, tb[par, second, :])
            mass = jnp.sum(ka.astype(F32), axis=1, keepdims=True) + jnp.sum(kb.astype(F32), axis=1, keepdims=True)
            t_own = tb[par, rows, :].astype(F32)
            upd = (drive + (2.0 / kern_width) * (mass * t_own - pull)) * (1.0 / n_total)
            th[rows, :] = th[rows, :] + step_size * upd

            @pl.when(jnp.logical_and(t < NUM_STEPS - 1, k > 0))
            def _():
                t_copy(1 - par, done).start()

            @pl.when(t == NUM_STEPS - 1)
            def _():
                dst = out_ref.at[pl.ds(pl.multiple_of((i % 2) * TILE, TILE), TILE), pl.ds(pl.multiple_of(z * width, BLK), width)]

                @pl.when(zz == z)
                def _():
                    pltpu.make_async_copy(th.at[rows, :], dst, out_s.at[i]).start()

                @pl.when(zz != z)
                def _():
                    rc(th.at[rows, :], dst, out_s.at[i], out_r.at[z, i % 2], dev(zz, y, c)).start()
            return cc

        lax.fori_loop(0, 8, phi_tile, 0)

        @pl.when(t < NUM_STEPS - 1)
        def _():
            _, done = tile_of(7)
            finish_rows(done, 1 - par)
            t_copy(1 - par, done).start()
            z_copy().start()

        for ch in range(KCH):
            for e in range(2):
                ky_copy(e, 0, ch, qf(y, e)).wait_send()

            @pl.when(is_end)
            def _(ch=ch):
                ky_copy(e2, 1, ch, qz(y, e2)).wait_send()
            for j in range(3):
                q2 = (qz(y, e2), qf(y, e2), qz(1 - y, e2))[j]
                q1 = (qz(y, e1), qf(y, e1), qz(1 - y, e1))[j]
                kc_copy(e2, j, ch, q2).wait_send()

                @pl.when(is_mid)
                def _(ch=ch, j=j, q1=q1):
                    kc_copy(e1, j, ch, q1).wait_send()
            for q in range(8):
                kx_copy(ch, q).wait_send()
        return carry

    lax.fori_loop(0, NUM_STEPS, step, 0)

    for k in range(1, 4):
        in_copy((z + k) % 4).wait_send()

    def out_wait(i, cc):
        zz = (i // 2 + 2 * c) % 4
        rows = pl.ds(pl.multiple_of(i * TILE, TILE), TILE)
        dst = out_ref.at[pl.ds(pl.multiple_of((i % 2) * TILE, TILE), TILE), pl.ds(pl.multiple_of(z * width, BLK), width)]

        @pl.when(zz == z)
        def _():
            pltpu.make_async_copy(th.at[rows, :], dst, out_s.at[i]).wait()

        @pl.when(zz != z)
        def _():
            rc(th.at[rows, :], dst, out_s.at[i], out_r.at[z, i % 2], dev(zz, y, c)).wait_send()
        return cc

    lax.fori_loop(0, 8, out_wait, 0)
    for k in range(1, 4):
        zz = (z + k) % 4
        for s in range(2):
            dst = out_ref.at[pl.ds(s * TILE, TILE), pl.ds(pl.multiple_of(zz * width, BLK), width)]
            rc(dst, dst, out_s.at[0], out_r.at[zz, s], me).wait_recv()


def solution(mesh):
    part_size = mesh.shape["part"]
    feat_size = mesh.shape["feat"]

    def local_steps(local_theta, prec_loc, mean_loc, factor_loc):
        rows_loc, feat_loc = local_theta.shape
        n_total = rows_loc * part_size
        feat_total = feat_loc * feat_size
        width = feat_loc // part_size
        kern_width = 2.0 * feat_total / math.log(n_total)
        step_size = 0.15 * n_total * feat_total / math.log(n_total)
        anym = pl.BlockSpec(memory_space=pl.ANY)
        dma = pltpu.SemaphoreType.DMA
        body = lambda *refs: _kernel(n_total, kern_width, step_size, *refs)
        return pl.pallas_call(
            body,
            out_shape=pltpu.VMEM((rows_loc, feat_loc), F32),
            in_specs=[anym, anym, anym, anym],
            out_specs=pl.BlockSpec(memory_space=pltpu.VMEM),
            scratch_shapes=[
                pltpu.VMEM((n_total, width), F32),
                pltpu.VMEM((2, n_total, width), BF),
                pltpu.VMEM((n_total, width), BF),
                pltpu.VMEM((n_total, width), BF),
                pltpu.VMEM((8, BLK, PW), F32),
                pltpu.VMEM((2, BLK, PW), F32),
                pltpu.VMEM((2, 3 * NCH, CH, PW), F32),
                pltpu.VMEM((BLK, PW), F32),
                pltpu.VMEM((2, 8, BLK, PW), BF),
                pltpu.VMEM((2, n_total // 2, n_total), BF),
                pltpu.VMEM((17, HR, BLK), F32),
                pltpu.VMEM((9, HR, BLK), F32),
                pltpu.VMEM((16, BLK), F32), pltpu.VMEM((16, BLK), F32), pltpu.VMEM((8, 16, BLK), F32),
                pltpu.VMEM((1, width), F32), pltpu.VMEM((1, width), F32),
                pltpu.VMEM((BLK, width), BF), pltpu.VMEM((BLK, width), BF),
                dma((4,)), dma((4,)), dma((8,)),
                dma((4,)), dma((4,)), dma((8,)), dma((8,)), dma, dma,
                dma((2, NCH)), dma((2, NCH)), dma((2, 3 * NCH)), dma((2, 3 * NCH)), dma((NCH,)), dma((NCH,)),
                dma((2, 3 * KCH)), dma((2, 3 * KCH)), dma((2, 2, KCH)), dma((2, 2, KCH)), dma((8, KCH)), dma((8, KCH)),
                dma((8,)), dma((4, 2)),
            ],
            compiler_params=pltpu.CompilerParams(collective_id=0, has_side_effects=True, vmem_limit_bytes=54 * 1024 * 1024),
            name="svgd",
        )(local_theta, prec_loc[None, :], mean_loc[None, :], factor_loc.T)

    row_spec = P(("ens", "part"), "feat")
    vec_spec = P(("ens", "feat"))
    fac_spec = P(("ens", "feat"), None)
    return jax.shard_map(local_steps, mesh=mesh, in_specs=(row_spec, vec_spec, vec_spec, fac_spec), out_specs=row_spec, check_vma=False)
```
